32 devices in a mesh: dp: 4 (over x, y), ep: 8 (over z, core).
Axes of the slice: x: 2, y: 2, z: 4, core: 2. Of those that a mesh axis runs over, the one named last changes fastest.
Arguments:
- x: bfloat16 [4, 8, 256, 3584], P('dp', 'ep'), parts along dimension 0
- expert: int32 [4, 8, 256, 2], P('dp', 'ep'), parts along dimension 0
- slot: int32 [4, 8, 256, 2], P('dp', 'ep'), parts along dimension 0
- gate: float32 [4, 8, 256, 2], P('dp', 'ep'), parts along dimension 0
- w_gate: bfloat16 [16, 3584, 4864], P('ep')
- w_up: bfloat16 [16, 3584, 4864], P('ep')
- w_down: bfloat16 [16, 4864, 3584], P('ep')
Outputs:
- y: bfloat16 [4, 8, 256, 3584], P('dp', 'ep'), parts along dimension 0
There are 4 independent parts. The reference program is written for one: setup_inputs(seed, part) draws one part's arguments, and reference() takes and returns one part's arrays. A program takes and returns all parts, laid end to end along the dimension named above; an argument that names none is the same for every part.
All inputs are finite; a program needn't handle non-finite values.
Results may differ from the reference program's by a relative error of at most 0.009.
Values are sent between devices in bfloat16 or wider.
A program may use at most 2 GiB of HBM per device.

```python
import jax
import jax.numpy as jnp

MEMBERS = 8
TOKENS = 256
D = 3584
FF = 4864
TOP = 2
EXPERTS = 16
SLOTS = 5 * TOKENS * TOP // (4 * EXPERTS)


def setup_inputs(seed: int = 0, part: int = 0) -> dict:
    own, k1, k2, k3, k4, k5, k6 = jax.random.split(jax.random.key(seed), 7)
    kx, ke, kl, kg = jax.random.split(jax.random.fold_in(own, part), 4)
    devices = (1, MEMBERS)
    place = jax.random.permutation(kl, jnp.arange(EXPERTS, dtype=jnp.uint32))
    slow = ((EXPERTS + (9 * place) % EXPERTS) << ((9 * place) // EXPERTS)) // EXPERTS
    wait = (jax.random.bits(ke, (*devices, TOKENS, EXPERTS), jnp.uint32) >> 10) * slow
    expert = jnp.argsort(wait, axis=-1)[..., :TOP].astype(jnp.int32)
    chosen = jax.nn.one_hot(expert, EXPERTS, dtype=jnp.int32)
    in_line = jnp.cumsum(chosen.reshape(*devices, TOKENS * TOP, EXPERTS), axis=2) - 1
    slot = jnp.sum(in_line.reshape(chosen.shape) * chosen, axis=-1)

    def one(key, rows, columns):
        return (jax.random.normal(key, (rows, columns), jnp.float32) * rows**-0.5).astype(jnp.bfloat16)

    def weights(key, rows, columns):
        return jax.lax.map(lambda k: one(k, rows, columns), jax.random.split(key, EXPERTS))

    return {
        "x": jax.random.normal(kx, (*devices, TOKENS, D), jnp.float32).astype(jnp.bfloat16),
        "expert": expert,
        "slot": slot,
        "gate": jax.nn.softmax(jax.random.normal(kg, expert.shape, jnp.float32)),
        "w_gate": weights(k1, D, FF),
        "w_up": weights(k2, D, FF),
        "w_down": weights(k3, FF, D),
    }


def einsum(form, a, b):
    return jnp.einsum(form, a.astype(jnp.float32), b.astype(jnp.float32))


def reference(x, expert, slot, gate, w_gate, w_up, w_down):
    to_expert = jax.nn.one_hot(expert, EXPERTS, dtype=jnp.bfloat16)
    to_slot = jax.nn.one_hot(slot, SLOTS, dtype=jnp.bfloat16)
    weighted = to_expert * gate[..., None].astype(jnp.bfloat16)
    dispatch = einsum("abtke,abtkc->abtec", to_expert, to_slot).astype(jnp.bfloat16)
    combine = einsum("abtke,abtkc->abtec", weighted, to_slot).astype(jnp.bfloat16)
    z = einsum("abtec,abtd->aebcd", dispatch, x).astype(jnp.bfloat16)
    h = jax.nn.silu(einsum("aebcd,edf->aebcf", z, w_gate))
    h = (h * einsum("aebcd,edf->aebcf", z, w_up)).astype(jnp.bfloat16)
    out = einsum("aebcf,efd->aebcd", h, w_down).astype(jnp.bfloat16)
    y = einsum("abtec,aebcd->abtd", combine, out)
    return y.astype(jnp.bfloat16)
```

```python
import functools

import jax
import jax.numpy as jnp
from jax import lax
from jax.experimental import pallas as pl
from jax.experimental.pallas import tpu as pltpu
from jax.sharding import PartitionSpec as P

MESH = pl.DeviceIdType.MESH
BF16, F32 = jnp.bfloat16, jnp.float32
CW = 256
KC = 512
AHEAD = 3
VMEM_BYTES = 66 * 1024 * 1024 - 2 * 1024 * 1024 - 65536


def dot(a, b):
    return jnp.dot(a, b, preferred_element_type=F32)


def dot_nt(a, b):
    return lax.dot_general(a, b, (((1,), (1,)), ((), ())), preferred_element_type=F32)


class Place:
    def __init__(self):
        self.dp = lax.axis_index("dp")
        self.ep = lax.axis_index("ep")
        self.z = lax.div(self.ep, 2)
        self.c = lax.rem(self.ep, 2)
        half = lax.div(self.z, 2)
        self.near = self.z + 1 - 2 * lax.rem(self.z, 2)
        self.far_inner = 2 - half
        self.far = [2 * (1 - half), 2 * (1 - half) + 1]
        self.inner = jnp.logical_or(self.z == 1, self.z == 2)
        self.end = jnp.logical_or(self.z == 0, self.z == 3)

    def dev(self, z, c):
        return (self.dp, 2 * z + c)

    def barrier(self):
        sem = pltpu.get_barrier_semaphore()
        for i in range(1, 8):
            peer = lax.rem(self.ep + i, 8)
            pl.semaphore_signal(sem, inc=1, device_id=(self.dp, peer), device_id_type=MESH)
        pl.semaphore_wait(sem, 7)


def route_kernel(slots, meta_ref, a_ref, cw_ref, pn_ref, pf_ref, qn_ref, qf_ref):
    me = Place()
    t = meta_ref.shape[2]
    e = [meta_ref[0], meta_ref[1]]
    s = [meta_ref[2], meta_ref[3]]
    g = [meta_ref[4], meta_ref[5]]
    src = lax.broadcasted_iota(jnp.int32, (8, t), 0)
    lane = lax.broadcasted_iota(jnp.int32, (8, t), 1)
    zs, cs = src // 2, src % 2
    near = zs + 1 - 2 * (zs % 2)
    inner, end = 2 - zs // 2, 3 - 3 * (zs // 2)
    chip = [jnp.floor(v * 0.25).astype(jnp.int32) for v in e]

    def needs(where):
        return jnp.logical_or(chip[0] == where, chip[1] == where)

    m_n, m_a = needs(near), needs(end)
    m_b = jnp.logical_and(needs(inner), jnp.logical_not(m_a))
    row = lax.broadcasted_iota(jnp.int32, (t, t), 0)
    col = lax.broadcasted_iota(jnp.int32, (t, t), 1)
    before = (row < col).astype(F32).astype(BF16)

    def count(mask):
        return dot(mask.astype(F32).astype(BF16), before).astype(jnp.int32)

    total_a = jnp.sum(m_a.astype(F32), axis=1, keepdims=True).astype(jnp.int32)
    pos_n = jnp.where(m_n, count(m_n), -1)
    pos_f = jnp.where(m_a, count(m_a), jnp.where(m_b, total_a + count(m_b), -1))
    pos = jnp.where(zs == me.z, lane, jnp.where(zs == me.near, pos_n, pos_f))

    codes = []
    for j in range(2):
        local = e[j].astype(jnp.int32) - 2 * me.ep
        hit = jnp.logical_and(local >= 0, local < 2)
        code = local * (2 * slots) + cs * slots + s[j].astype(jnp.int32) + 1
        codes.append(jnp.where(hit, code, 0).astype(F32))
    table = jnp.concatenate(codes + g, axis=0).astype(BF16)
    slot_row = lax.broadcasted_iota(jnp.int32, (4 * slots, t), 0) + 1
    slot_col = lax.broadcasted_iota(jnp.int32, (t, 4 * slots), 1) + 1
    for k in range(8):
        perm = (row == pos[k : k + 1]).astype(F32).astype(BF16)
        by_row = dot_nt(table, perm)
        by_col = dot_nt(perm, table)
        r0 = by_row[k : k + 1].astype(jnp.int32)
        r1 = by_row[8 + k : 9 + k].astype(jnp.int32)
        c0 = by_col[:, k : k + 1].astype(jnp.int32)
        c1 = by_col[:, 8 + k : 9 + k].astype(jnp.int32)
        g0, g1 = by_col[:, 16 + k : 17 + k], by_col[:, 24 + k : 25 + k]
        hit = jnp.logical_or(slot_row == r0, slot_row == r1)
        place = slice((k % 2) * t, (k % 2 + 1) * t)
        a_ref[k // 2, :, place] = hit.astype(F32).astype(BF16)
        weight = jnp.where(slot_col == c0, g0, 0.0) + jnp.where(slot_col == c1, g1, 0.0)
        cw_ref[k // 2, place, :] = weight.astype(BF16)

    eye = (row == col).astype(F32).astype(BF16)
    for pos_x, p_ref, q_ref in ((pos_n, pn_ref, qn_ref), (pos_f, pf_ref, qf_ref)):
        mine = jnp.sum(jnp.where(src == me.ep, pos_x, 0).astype(F32), axis=0, keepdims=True)
        p_ref[...] = (row == mine.astype(jnp.int32)).astype(F32).astype(BF16)
        column = dot_nt(eye, jnp.broadcast_to(mine, (8, t)).astype(BF16))[:, 0:1]
        q_ref[...] = (col == column.astype(jnp.int32)).astype(F32).astype(BF16)


def up_kernel(far_rows, end_rows, x_ref, a_ref, pn_ref, pf_ref, wg_hbm, wu_hbm, h_ref, xall, sn, sf, zbuf, gacc, uacc, wgb, wub, wsem, send_sem, recv_sem):
    me = Place()
    t, d = x_ref.shape
    ff = wg_hbm.shape[2]
    rows = zbuf.shape[1]
    n, nk = d // CW, d // KC
    tiles = ff // CW
    parts = wgb.shape[0]
    sizes = [tiles // parts + (i < tiles % parts) for i in range(parts)]
    starts = [sum(sizes[:i]) for i in range(parts)]

    def weights(u, p):
        e, k = lax.rem(u, 2), lax.div(u, 2)
        for i, (hbm, buf) in enumerate(((wg_hbm, wgb), (wu_hbm, wub))):
            yield pltpu.make_async_copy(
                hbm.at[e, pl.ds(pl.multiple_of(k * KC, KC), KC), pl.ds(starts[p] * CW, sizes[p] * CW)],
                buf.at[p, :, pl.ds(0, sizes[p] * CW)],
                wsem.at[p, i],
            )

    for p in range(parts - 1):
        for copy in weights(0, p):
            copy.start()

    def clear(j, _):
        xall[j] = jnp.zeros(xall.shape[1:], BF16)
        return 0

    lax.fori_loop(0, n, clear, 0)
    me.barrier()

    def cell(j, slot, count):
        return xall.at[j, pl.ds(pl.multiple_of(slot * t, t), count)]

    def remote(j, kind, src, slot, count, to):
        return pltpu.make_async_remote_copy(
            src_ref=src,
            dst_ref=cell(j, slot, count),
            send_sem=send_sem.at[j, kind],
            recv_sem=recv_sem.at[j, slot],
            device_id=to,
            device_id_type=MESH,
        )

    partner, nearby = me.dev(me.z, 1 - me.c), me.dev(me.near, me.c)
    own, near_slot = me.ep, 2 * me.near + me.c
    far_slots = [2 * f + me.c for f in me.far]

    def sends(j):
        cols = pl.ds(pl.multiple_of(j * CW, CW), CW)
        yield remote(j, 2, sf.at[j], own, far_rows, me.dev(me.far_inner, me.c))
        yield remote(j, 1, sn.at[j], own, end_rows, nearby)
        yield remote(j, 0, x_ref.at[:, cols], own, t, partner)

    def forward(j, kind, slot, count, to):
        return remote(j, kind, cell(j, slot, count), slot, count, to)

    def arrived(j, slot, count):
        forward(j, 0, slot, count, partner).wait_recv()

    def pack(j, _):
        cols = pl.ds(pl.multiple_of(j * CW, CW), CW)
        block = x_ref[:, cols]
        sf[j] = dot(pf_ref[:far_rows], block).astype(BF16)
        sn[j] = dot(pn_ref[:end_rows], block).astype(BF16)
        xall[j, pl.ds(pl.multiple_of(own * t, t), t)] = block
        for copy in sends(j):
            copy.start()
        return 0

    lax.fori_loop(0, AHEAD, pack, 0)

    def clear_sums(i, _):
        cols = pl.ds(pl.multiple_of(i * CW, CW), CW)
        for e in range(2):
            gacc[e, :, cols] = jnp.zeros((rows, CW), F32)
            uacc[e, :, cols] = jnp.zeros((rows, CW), F32)
        return 0

    lax.fori_loop(0, tiles, clear_sums, 0)

    def gather(k):
        for i in range(2):
            j = 2 * k + i
            arrived(j, 2 * me.z + 1 - me.c, t)
            arrived(j, 2 * me.near + 1 - me.c, end_rows)
            for f in me.far:

                @pl.when(me.inner)
                def _():
                    arrived(j, 2 * f + 1 - me.c, far_rows)

                @pl.when(me.end)
                def _():
                    arrived(j, 2 * f + 1 - me.c, end_rows)

            for zs in range(4):
                block = dot(a_ref[zs], xall[j, zs * 2 * t : (zs + 1) * 2 * t]).astype(BF16)
                size = rows // 4
                for e in range(2):
                    zbuf[e, zs * size : (zs + 1) * size, i * CW : (i + 1) * CW] = block[e * size : (e + 1) * size]

    def unit(u):
        e, k = lax.rem(u, 2), lax.div(u, 2)

        @pl.when(e == 0)
        def _():
            gather(k)

        for p in range(parts):
            for copy in weights(u, p):
                copy.wait()
            later, q = (u, p + parts - 1) if p == 0 else (u + 1, p - 1)

            @pl.when(later < 2 * nk)
            def _():
                for copy in weights(later, q):
                    copy.start()

            def tile(i, last):
                here = pl.ds(pl.multiple_of(i * CW, CW), CW)
                cols = pl.ds(pl.multiple_of((starts[p] + i) * CW, CW), CW)
                z = zbuf[e]
                gate = gacc[e, :, cols] + dot(z, wgb[p, :, here])
                up = uacc[e, :, cols] + dot(z, wub[p, :, here])
                if last:
                    h_ref[e, :, cols] = (gate * jax.nn.sigmoid(gate) * up).astype(BF16)
                else:
                    gacc[e, :, cols] = gate
                    uacc[e, :, cols] = up
                return 0

            @pl.when(k < nk - 1)
            def _():
                lax.fori_loop(0, sizes[p], lambda i, _: tile(i, False), 0)

            @pl.when(k == nk - 1)
            def _():
                lax.fori_loop(0, sizes[p], lambda i, _: tile(i, True), 0)

    def step(j, _):
        @pl.when(j + AHEAD < n)
        def _():
            pack(j + AHEAD, 0)

        @pl.when(j < n)
        def _():
            @pl.when(me.inner)
            def _():
                for i, slot in enumerate(far_slots):
                    arrived(j, slot, far_rows)
                    forward(j, 6 + i, slot, end_rows, nearby).start()
                    forward(j, 4 + i, slot, far_rows, partner).start()

            arrived(j, near_slot, end_rows)
            forward(j, 3, near_slot, end_rows, partner).start()

        @pl.when(jnp.logical_and(me.end, jnp.logical_and(j >= 1, j <= n)))
        def _():
            for i, slot in enumerate(far_slots):
                arrived(j - 1, slot, end_rows)
                forward(j - 1, 4 + i, slot, end_rows, partner).start()

        @pl.when(j >= 3)
        def _():
            unit(j - 3)

        return 0

    lax.fori_loop(0, n + 3, step, 0)

    def drain(j, _):
        for copy in sends(j):
            copy.wait_send()
        forward(j, 3, near_slot, end_rows, partner).wait_send()

        @pl.when(me.inner)
        def _():
            for i, slot in enumerate(far_slots):
                forward(j, 6 + i, slot, end_rows, nearby).wait_send()
                forward(j, 4 + i, slot, far_rows, partner).wait_send()

        @pl.when(me.end)
        def _():
            for i, slot in enumerate(far_slots):
                forward(j, 4 + i, slot, end_rows, partner).wait_send()

        return 0

    lax.fori_loop(0, n, drain, 0)


def down_kernel(far_rows, end_rows, h_ref, cw_ref, qn_ref, qf_ref, wd_hbm, y_ref, o, yd, yn, yf, yr, sd, sn, sf, wdb, wsem, send_sem, dsem, nsem, fsem, rsem):
    me = Place()
    t, d = y_ref.shape
    ff = wd_hbm.shape[1]
    rows = h_ref.shape[1]
    size = rows // 4
    n = d // CW
    depth = wdb.shape[0]
    lag = 5

    def weights(q):
        cols = pl.ds(pl.multiple_of(q * CW, CW), CW)
        slot = lax.rem(q, depth)
        for e in range(2):
            yield pltpu.make_async_copy(wd_hbm.at[e, :, cols], wdb.at[slot, e], wsem.at[slot, e])

    for q in range(depth - 1):
        for copy in weights(q):
            copy.start()
    me.barrier()

    partner, nearby = me.dev(me.z, 1 - me.c), me.dev(me.near, me.c)

    def remote(q, kind, src, dst, recv, to):
        return pltpu.make_async_remote_copy(
            src_ref=src, dst_ref=dst, send_sem=send_sem.at[q, kind], recv_sem=recv, device_id=to, device_id_type=MESH
        )

    def to_partner(q):
        return remote(q, 0, sd.at[q], yd.at[q], dsem.at[q], partner)

    def to_near(q):
        return remote(q, 1, sn.at[q], yn.at[q], nsem.at[q], nearby)

    def relay(q, i):
        return remote(q, 2 + i, sf.at[q, i, pl.ds(0, end_rows)], yr.at[q, i], rsem.at[q, i], nearby)

    def to_far(q, i):
        return remote(q, 2 + i, sf.at[q, i], yf.at[q], fsem.at[q], me.dev(me.far[i], me.c))

    def part(q, zs, c, count):
        return dot(cw_ref[zs, pl.ds(pl.multiple_of(c * t, t), count), :], o[q, zs])

    def both(q, zs, count):
        other = yd[q, pl.ds(pl.multiple_of(zs * t, t), count)].astype(F32)
        return part(q, zs, me.c, count) + other

    def step(q, _):
        @pl.when(q < n)
        def _():
            for copy in weights(q):
                copy.wait()

            @pl.when(q + depth - 1 < n)
            def _():
                for copy in weights(q + depth - 1):
                    copy.start()

            slot = lax.rem(q, depth)
            for e in range(2):
                block = dot(h_ref[e], wdb[slot, e]).astype(BF16)
                for zs in range(4):
                    o[q, zs, e * size : (e + 1) * size] = block[zs * size : (zs + 1) * size]
            for zs in range(4):
                sd[q, zs * t : (zs + 1) * t] = part(q, zs, 1 - me.c, t).astype(BF16)
            to_partner(q).start()

        @pl.when(jnp.logical_and(q >= 1, q <= n))
        def _():
            r = q - 1
            to_partner(r).wait_recv()

            @pl.when(me.end)
            def _():
                for i, f in enumerate(me.far):
                    sf[r, i, 0:end_rows] = both(r, f, end_rows).astype(BF16)
                    relay(r, i).start()

            sn[r] = both(r, me.near, end_rows).astype(BF16)
            to_near(r).start()

        @pl.when(jnp.logical_and(me.inner, jnp.logical_and(q >= 2, q <= n + 1)))
        def _():
            r = q - 2
            for i, f in enumerate(me.far):
                relay(r, i).wait_recv()
                total = both(r, f, far_rows)
                sf[r, i, 0:end_rows] = (total[:end_rows] + yr[r, i].astype(F32)).astype(BF16)
                if far_rows > end_rows:
                    sf[r, i, end_rows:far_rows] = total[end_rows:].astype(BF16)
                to_far(r, i).start()

        @pl.when(q >= lag)
        def _():
            r = q - lag
            to_near(r).wait_recv()
            to_far(r, 0).wait_recv()
            total = both(r, me.z, t)
            total += dot(qn_ref[:, :end_rows], yn[r])
            total += dot(qf_ref[:, :far_rows], yf[r])
            y_ref[:, pl.ds(pl.multiple_of(r * CW, CW), CW)] = total.astype(BF16)

        return 0

    lax.fori_loop(0, n + lag, step, 0)

    def drain(q, _):
        to_partner(q).wait_send()
        to_near(q).wait_send()

        @pl.when(me.end)
        def _():
            for i in range(2):
                relay(q, i).wait_send()

        @pl.when(me.inner)
        def _():
            for i in range(2):
                to_far(q, i).wait_send()

        return 0

    lax.fori_loop(0, n, drain, 0)


def up_call(x, a, pn, pf, w_gate, w_up, slots, far_rows, end_rows, ident):
    t, d = x.shape
    ff = w_gate.shape[2]
    n, rows = d // CW, 8 * slots
    tiles = ff // CW
    parts = min(4, tiles)
    wide = -(-tiles // parts) * CW
    vmem, hbm = pl.BlockSpec(memory_space=pltpu.VMEM), pl.BlockSpec(memory_space=pl.ANY)
    return pl.pallas_call(
        functools.partial(up_kernel, far_rows, end_rows),
        out_shape=jax.ShapeDtypeStruct((2, rows, ff), BF16),
        in_specs=[vmem] * 4 + [hbm] * 2,
        out_specs=vmem,
        scratch_shapes=[
            pltpu.VMEM((n, 8 * t, CW), BF16),
            pltpu.VMEM((n, end_rows, CW), BF16),
            pltpu.VMEM((n, far_rows, CW), BF16),
            pltpu.VMEM((2, rows, KC), BF16),
            pltpu.VMEM((2, rows, ff), F32),
            pltpu.VMEM((2, rows, ff), F32),
            pltpu.VMEM((parts, KC, wide), BF16),
            pltpu.VMEM((parts, KC, wide), BF16),
            pltpu.SemaphoreType.DMA((parts, 2)),
            pltpu.SemaphoreType.DMA((n, 8)),
            pltpu.SemaphoreType.DMA((n, 8)),
        ],
        compiler_params=pltpu.CompilerParams(collective_id=ident, has_side_effects=True, vmem_limit_bytes=VMEM_BYTES),
        name=f"up_{far_rows}_{end_rows}",
    )(x, a, pn, pf, w_gate, w_up)


def down_call(h, cw, qn, qf, w_down, far_rows, end_rows, ident):
    _, rows, ff = h.shape
    d, t = w_down.shape[2], qn.shape[0]
    n = d // CW
    vmem, hbm = pl.BlockSpec(memory_space=pltpu.VMEM), pl.BlockSpec(memory_space=pl.ANY)
    return pl.pallas_call(
        functools.partial(down_kernel, far_rows, end_rows),
        out_shape=jax.ShapeDtypeStruct((t, d), BF16),
        in_specs=[vmem] * 4 + [hbm],
        out_specs=vmem,
        scratch_shapes=[
            pltpu.VMEM((n, 4, rows // 2, CW), BF16),
            pltpu.VMEM((n, 4 * t, CW), BF16),
            pltpu.VMEM((n, end_rows, CW), BF16),
            pltpu.VMEM((n, far_rows, CW), BF16),
            pltpu.VMEM((n, 2, end_rows, CW), BF16),
            pltpu.VMEM((n, 4 * t, CW), BF16),
            pltpu.VMEM((n, end_rows, CW), BF16),
            pltpu.VMEM((n, 2, far_rows, CW), BF16),
            pltpu.VMEM((3, 2, ff, CW), BF16),
            pltpu.SemaphoreType.DMA((3, 2)),
            pltpu.SemaphoreType.DMA((n, 4)),
            pltpu.SemaphoreType.DMA((n,)),
            pltpu.SemaphoreType.DMA((n,)),
            pltpu.SemaphoreType.DMA((n,)),
            pltpu.SemaphoreType.DMA((n, 2)),
        ],
        compiler_params=pltpu.CompilerParams(collective_id=ident, has_side_effects=True, vmem_limit_bytes=VMEM_BYTES),
        name=f"down_{far_rows}_{end_rows}",
    )(h, cw, qn, qf, w_down)


def route_call(meta, slots):
    t = meta.shape[2]
    vmem = pl.BlockSpec(memory_space=pltpu.VMEM)
    square = jax.ShapeDtypeStruct((t, t), BF16)
    return pl.pallas_call(
        functools.partial(route_kernel, slots),
        out_shape=[
            jax.ShapeDtypeStruct((4, 4 * slots, 2 * t), BF16),
            jax.ShapeDtypeStruct((4, 2 * t, 4 * slots), BF16),
            square,
            square,
            square,
            square,
        ],
        in_specs=[vmem],
        out_specs=[vmem] * 6,
        name="route",
    )(meta)


def solution(mesh):
    def body(x, expert, slot, gate, w_gate, w_up, w_down):
        x, expert, slot, gate = x[0, 0], expert[0, 0], slot[0, 0], gate[0, 0]
        t = x.shape[0]
        slots = 5 * t * 2 // (4 * 16)
        kept = jnp.where(slot < slots, expert, -1)
        meta = jnp.concatenate([kept.T.astype(F32), jnp.minimum(slot, slots).T.astype(F32), gate.T], axis=0)
        meta = lax.all_gather(meta, "ep", axis=1)
        a, cw, pn, pf, qn, qf = route_call(meta, slots)
        far_rows, end_rows = t, 4 * slots
        h = up_call(x, a, pn, pf, w_gate, w_up, slots, far_rows, end_rows, 1)
        y = down_call(h, cw, qn, qf, w_down, far_rows, end_rows, 2)
        return y[None, None]

    data, weight = P("dp", "ep", None, None), P("ep", None, None)
    return jax.shard_map(
        body,
        mesh=mesh,
        in_specs=(data, data, data, data, weight, weight, weight),
        out_specs=data,
        check_vma=False,
    )
```

```python
import functools

import jax
import jax.numpy as jnp
from jax import lax
from jax.experimental import pallas as pl
from jax.experimental.pallas import tpu as pltpu
from jax.sharding import PartitionSpec as P

MESH = pl.DeviceIdType.MESH
BF16, F32 = jnp.bfloat16, jnp.float32
CW = 256
KC = 512
AHEAD = 3
VMEM_BYTES = 66 * 1024 * 1024 - 2 * 1024 * 1024 - 65536


def dot(a, b):
    return jnp.dot(a, b, preferred_element_type=F32)


def dot_nt(a, b):
    return lax.dot_general(a, b, (((1,), (1,)), ((), ())), preferred_element_type=F32)


class Place:
    def __init__(self):
        self.dp = lax.axis_index("dp")
        self.ep = lax.axis_index("ep")
        self.z = lax.div(self.ep, 2)
        self.c = lax.rem(self.ep, 2)
        half = lax.div(self.z, 2)
        self.near = self.z + 1 - 2 * lax.rem(self.z, 2)
        self.far_inner = 2 - half
        self.far = [2 * (1 - half), 2 * (1 - half) + 1]
        self.inner = jnp.logical_or(self.z == 1, self.z == 2)
        self.end = jnp.logical_or(self.z == 0, self.z == 3)

    def dev(self, z, c):
        return (self.dp, 2 * z + c)

    def barrier(self):
        sem = pltpu.get_barrier_semaphore()
        for i in range(1, 8):
            peer = lax.rem(self.ep + i, 8)
            pl.semaphore_signal(sem, inc=1, device_id=(self.dp, peer), device_id_type=MESH)
        pl.semaphore_wait(sem, 7)


def route_kernel(slots, sizes, several, expert_ref, slot_ref, gate_ref, a_ref, cw_ref, pn_ref, pf_ref, qn_ref, qf_ref, pick_ref, mine, every, top, tops, send_sem, recv_sem, top_send, top_recv):
    me = Place()
    t = expert_ref.shape[1]
    slot = slot_ref[...]
    mine[0:2] = jnp.where(slot < slots, expert_ref[...], -1).astype(F32)
    mine[2:4] = jnp.minimum(slot, slots).astype(F32)
    mine[4:6] = gate_ref[...]
    mine[6:8] = jnp.zeros((2, t), F32)

    barrier = pltpu.get_barrier_semaphore()
    peers = [(me.dp, lax.rem(me.ep + i, 8)) for i in range(1, 8)]
    groups = [(lax.rem(me.dp + i, 4), me.ep) for i in range(1, 4)]
    if not several:
        groups = []
    for peer in peers + groups:
        pl.semaphore_signal(barrier, inc=1, device_id=peer, device_id_type=MESH)
    pl.semaphore_wait(barrier, len(peers) + len(groups))

    def table_to(i):
        return pltpu.make_async_remote_copy(
            src_ref=mine,
            dst_ref=every.at[me.ep],
            send_sem=send_sem.at[i],
            recv_sem=recv_sem.at[me.ep],
            device_id=peers[i],
            device_id_type=MESH,
        )

    def table_from(i):
        source = lax.rem(me.ep + 8 - i, 8)
        return pltpu.make_async_remote_copy(
            src_ref=mine,
            dst_ref=every.at[source],
            send_sem=send_sem.at[0],
            recv_sem=recv_sem.at[source],
            device_id=peers[0],
            device_id_type=MESH,
        )

    for i in range(7):
        table_to(i).start()
    every[me.ep] = mine[...]
    for i in range(1, 8):
        table_from(i).wait_recv()

    e = [every[:, 0, :], every[:, 1, :]]
    s = [every[:, 2, :], every[:, 3, :]]
    g = [every[:, 4, :], every[:, 5, :]]
    src = lax.broadcasted_iota(jnp.int32, (8, t), 0)
    lane = lax.broadcasted_iota(jnp.int32, (8, t), 1)
    zs, cs = src // 2, src % 2
    near = zs + 1 - 2 * (zs % 2)
    inner, end = 2 - zs // 2, 3 - 3 * (zs // 2)
    chip = [jnp.floor(v * 0.25).astype(jnp.int32) for v in e]

    def needs(where):
        return jnp.logical_or(chip[0] == where, chip[1] == where)

    m_n, m_a = needs(near), needs(end)
    m_b = jnp.logical_and(needs(inner), jnp.logical_not(m_a))
    row = lax.broadcasted_iota(jnp.int32, (t, t), 0)
    col = lax.broadcasted_iota(jnp.int32, (t, t), 1)
    before = (row < col).astype(F32).astype(BF16)

    def count(mask):
        return dot(mask.astype(F32).astype(BF16), before).astype(jnp.int32)

    total_a = jnp.sum(m_a.astype(F32), axis=1, keepdims=True).astype(jnp.int32)
    pos_n = jnp.where(m_n, count(m_n), -1)
    pos_f = jnp.where(m_a, count(m_a), jnp.where(m_b, total_a + count(m_b), -1))
    def most(mask):
        return jnp.max(jnp.sum(mask.astype(F32), axis=1, keepdims=True), axis=0, keepdims=True)

    far_top = most(jnp.logical_or(m_a, m_b))
    end_top = jnp.maximum(most(m_a), most(m_n))
    which = lax.broadcasted_iota(jnp.int32, (8, 128), 0)
    top[...] = jnp.where(which == 0, far_top, end_top)

    def top_copy(i, slot):
        return pltpu.make_async_remote_copy(
            src_ref=top,
            dst_ref=tops.at[slot],
            send_sem=top_send.at[i],
            recv_sem=top_recv.at[slot],
            device_id=groups[i],
            device_id_type=MESH,
        )

    for i in range(len(groups)):
        top_copy(i, i).start()

    pos = jnp.where(zs == me.z, lane, jnp.where(zs == me.near, pos_n, pos_f))

    codes = []
    for j in range(2):
        local = e[j].astype(jnp.int32) - 2 * me.ep
        hit = jnp.logical_and(local >= 0, local < 2)
        code = local * (2 * slots) + cs * slots + s[j].astype(jnp.int32) + 1
        codes.append(jnp.where(hit, code, 0).astype(F32))
    table = jnp.concatenate(codes + g, axis=0).astype(BF16)
    slot_row = lax.broadcasted_iota(jnp.int32, (4 * slots, t), 0) + 1
    slot_col = lax.broadcasted_iota(jnp.int32, (t, 4 * slots), 1) + 1
    for k in range(8):
        perm = (row == pos[k : k + 1]).astype(F32).astype(BF16)
        by_row = dot_nt(table, perm)
        by_col = dot_nt(perm, table)
        r0 = by_row[k : k + 1].astype(jnp.int32)
        r1 = by_row[8 + k : 9 + k].astype(jnp.int32)
        c0 = by_col[:, k : k + 1].astype(jnp.int32)
        c1 = by_col[:, 8 + k : 9 + k].astype(jnp.int32)
        g0, g1 = by_col[:, 16 + k : 17 + k], by_col[:, 24 + k : 25 + k]
        hit = jnp.logical_or(slot_row == r0, slot_row == r1)
        place = slice((k % 2) * t, (k % 2 + 1) * t)
        a_ref[k // 2, :, place] = hit.astype(F32).astype(BF16)
        weight = jnp.where(slot_col == c0, g0, 0.0) + jnp.where(slot_col == c1, g1, 0.0)
        cw_ref[k // 2, place, :] = weight.astype(BF16)

    eye = (row == col).astype(F32).astype(BF16)
    for pos_x, p_ref, q_ref in ((pos_n, pn_ref, qn_ref), (pos_f, pf_ref, qf_ref)):
        order = jnp.sum(jnp.where(src == me.ep, pos_x, 0).astype(F32), axis=0, keepdims=True)
        p_ref[...] = (row == order.astype(jnp.int32)).astype(F32).astype(BF16)
        column = dot_nt(eye, jnp.broadcast_to(order, (8, t)).astype(BF16))[:, 0:1]
        q_ref[...] = (col == column.astype(jnp.int32)).astype(F32).astype(BF16)

    limit = top[...]
    for i in range(len(groups)):
        top_copy(i, i).wait_recv()
        limit = jnp.maximum(limit, tops[i])
    far_max, end_max = limit[0:1], limit[1:2]
    pick = jnp.full((1, 128), len(sizes) - 1, jnp.int32)
    for i, (far_rows, end_rows) in reversed(list(enumerate(sizes[:-1]))):
        pick = jnp.where(jnp.logical_and(far_max <= far_rows, end_max <= end_rows), i, pick)
    pick_ref[...] = jnp.broadcast_to(pick, (8, 128))
    for i in range(7):
        table_to(i).wait_send()
    for i in range(len(groups)):
        top_copy(i, i).wait_send()


def up_kernel(far_rows, end_rows, x_ref, a_ref, pn_ref, pf_ref, wg_hbm, wu_hbm, h_ref, xall, sn, sf, zbuf, gacc, uacc, wgb, wub, wsem, send_sem, recv_sem):
    me = Place()
    t, d = x_ref.shape
    ff = wg_hbm.shape[2]
    rows = zbuf.shape[1]
    n, nk = d // CW, d // KC
    tiles = ff // CW
    parts = wgb.shape[0]
    sizes = [tiles // parts + (i < tiles % parts) for i in range(parts)]
    starts = [sum(sizes[:i]) for i in range(parts)]

    def weights(u, p):
        e, k = lax.rem(u, 2), lax.div(u, 2)
        for i, (hbm, buf) in enumerate(((wg_hbm, wgb), (wu_hbm, wub))):
            yield pltpu.make_async_copy(
                hbm.at[e, pl.ds(pl.multiple_of(k * KC, KC), KC), pl.ds(starts[p] * CW, sizes[p] * CW)],
                buf.at[p, :, pl.ds(0, sizes[p] * CW)],
                wsem.at[p, i],
            )

    for p in range(parts - 1):
        for copy in weights(0, p):
            copy.start()

    def clear(j, _):
        xall[j] = jnp.zeros(xall.shape[1:], BF16)
        return 0

    lax.fori_loop(0, n, clear, 0)
    me.barrier()

    def cell(j, slot, count):
        return xall.at[j, pl.ds(pl.multiple_of(slot * t, t), count)]

    def remote(j, kind, src, slot, count, to):
        return pltpu.make_async_remote_copy(
            src_ref=src,
            dst_ref=cell(j, slot, count),
            send_sem=send_sem.at[j, kind],
            recv_sem=recv_sem.at[j, slot],
            device_id=to,
            device_id_type=MESH,
        )

    partner, nearby = me.dev(me.z, 1 - me.c), me.dev(me.near, me.c)
    own, near_slot = me.ep, 2 * me.near + me.c
    far_slots = [2 * f + me.c for f in me.far]

    def sends(j):
        cols = pl.ds(pl.multiple_of(j * CW, CW), CW)
        yield remote(j, 2, sf.at[j], own, far_rows, me.dev(me.far_inner, me.c))
        yield remote(j, 1, sn.at[j], own, end_rows, nearby)
        yield remote(j, 0, x_ref.at[:, cols], own, t, partner)

    def forward(j, kind, slot, count, to):
        return remote(j, kind, cell(j, slot, count), slot, count, to)

    def arrived(j, slot, count):
        forward(j, 0, slot, count, partner).wait_recv()

    def pack(j, _):
        cols = pl.ds(pl.multiple_of(j * CW, CW), CW)
        block = x_ref[:, cols]
        sf[j] = dot(pf_ref[:far_rows], block).astype(BF16)
        sn[j] = dot(pn_ref[:end_rows], block).astype(BF16)
        xall[j, pl.ds(pl.multiple_of(own * t, t), t)] = block
        for copy in sends(j):
            copy.start()
        return 0

    lax.fori_loop(0, AHEAD, pack, 0)

    def clear_sums(i, _):
        cols = pl.ds(pl.multiple_of(i * CW, CW), CW)
        for e in range(2):
            gacc[e, :, cols] = jnp.zeros((rows, CW), F32)
            uacc[e, :, cols] = jnp.zeros((rows, CW), F32)
        return 0

    lax.fori_loop(0, tiles, clear_sums, 0)

    def gather(k):
        for i in range(2):
            j = 2 * k + i
            arrived(j, 2 * me.z + 1 - me.c, t)
            arrived(j, 2 * me.near + 1 - me.c, end_rows)
            for f in me.far:

                @pl.when(me.inner)
                def _():
                    arrived(j, 2 * f + 1 - me.c, far_rows)

                @pl.when(me.end)
                def _():
                    arrived(j, 2 * f + 1 - me.c, end_rows)

            for zs in range(4):
                block = dot(a_ref[zs], xall[j, zs * 2 * t : (zs + 1) * 2 * t]).astype(BF16)
                size = rows // 4
                for e in range(2):
                    zbuf[e, zs * size : (zs + 1) * size, i * CW : (i + 1) * CW] = block[e * size : (e + 1) * size]

    def unit(u):
        e, k = lax.rem(u, 2), lax.div(u, 2)

        @pl.when(e == 0)
        def _():
            gather(k)

        def tiles_of(p, last):
            for copy in weights(u, p):
                copy.wait()
            later, q = (u, p + parts - 1) if p == 0 else (u + 1, p - 1)

            def start():
                for copy in weights(later, q):
                    copy.start()

            if p > 0 and last:
                pl.when(later < 2 * nk)(start)
            else:
                start()
            for i in range(sizes[p]):
                here = pl.ds(i * CW, CW)
                cols = pl.ds((starts[p] + i) * CW, CW)
                z = zbuf[e]
                gate = gacc[e, :, cols] + dot(z, wgb[p, :, here])
                up = uacc[e, :, cols] + dot(z, wub[p, :, here])
                if last:
                    h_ref[e, :, cols] = (gate * jax.nn.sigmoid(gate) * up).astype(BF16)
                else:
                    gacc[e, :, cols] = gate
                    uacc[e, :, cols] = up

        @pl.when(k < nk - 1)
        def _():
            for p in range(parts):
                tiles_of(p, False)

        @pl.when(k == nk - 1)
        def _():
            for p in range(parts):
                tiles_of(p, True)

    def step(j, _):
        @pl.when(j + AHEAD < n)
        def _():
            pack(j + AHEAD, 0)

        @pl.when(j < n)
        def _():
            @pl.when(me.inner)
            def _():
                for i, slot in enumerate(far_slots):
                    arrived(j, slot, far_rows)
                    forward(j, 6 + i, slot, end_rows, nearby).start()
                    forward(j, 4 + i, slot, far_rows, partner).start()

            arrived(j, near_slot, end_rows)
            forward(j, 3, near_slot, end_rows, partner).start()

        @pl.when(jnp.logical_and(me.end, jnp.logical_and(j >= 1, j <= n)))
        def _():
            for i, slot in enumerate(far_slots):
                arrived(j - 1, slot, end_rows)
                forward(j - 1, 4 + i, slot, end_rows, partner).start()

        @pl.when(j >= 3)
        def _():
            unit(j - 3)

        return 0

    lax.fori_loop(0, n + 3, step, 0)

    def drain(j, _):
        for copy in sends(j):
            copy.wait_send()
        forward(j, 3, near_slot, end_rows, partner).wait_send()

        @pl.when(me.inner)
        def _():
            for i, slot in enumerate(far_slots):
                forward(j, 6 + i, slot, end_rows, nearby).wait_send()
                forward(j, 4 + i, slot, far_rows, partner).wait_send()

        @pl.when(me.end)
        def _():
            for i, slot in enumerate(far_slots):
                forward(j, 4 + i, slot, end_rows, partner).wait_send()

        return 0

    lax.fori_loop(0, n, drain, 0)


def down_kernel(far_rows, end_rows, h_ref, cw_ref, qn_ref, qf_ref, wd_hbm, y_ref, o, yd, yn, yf, yr, sd, sn, sf, wdb, wsem, send_sem, dsem, nsem, fsem, rsem):
    me = Place()
    t, d = y_ref.shape
    ff = wd_hbm.shape[1]
    rows = h_ref.shape[1]
    size = rows // 4
    n = d // CW
    depth = wdb.shape[0]
    lag = 5

    def weights(q):
        cols = pl.ds(pl.multiple_of(q * CW, CW), CW)
        slot = lax.rem(q, depth)
        for e in range(2):
            yield pltpu.make_async_copy(wd_hbm.at[e, :, cols], wdb.at[slot, e], wsem.at[slot, e])

    for q in range(depth - 1):
        for copy in weights(q):
            copy.start()
    me.barrier()

    partner, nearby = me.dev(me.z, 1 - me.c), me.dev(me.near, me.c)

    def remote(q, kind, src, dst, recv, to):
        return pltpu.make_async_remote_copy(
            src_ref=src, dst_ref=dst, send_sem=send_sem.at[q, kind], recv_sem=recv, device_id=to, device_id_type=MESH
        )

    def to_partner(q):
        return remote(q, 0, sd.at[q], yd.at[q], dsem.at[q], partner)

    def to_near(q):
        return remote(q, 1, sn.at[q], yn.at[q], nsem.at[q], nearby)

    def relay(q, i):
        return remote(q, 2 + i, sf.at[q, i, pl.ds(0, end_rows)], yr.at[q, i], rsem.at[q, i], nearby)

    def to_far(q, i):
        return remote(q, 2 + i, sf.at[q, i], yf.at[q], fsem.at[q], me.dev(me.far[i], me.c))

    def part(q, zs, c, count):
        return dot(cw_ref[zs, pl.ds(pl.multiple_of(c * t, t), count), :], o[q, zs])

    def both(q, zs, count):
        other = yd[q, pl.ds(pl.multiple_of(zs * t, t), count)].astype(F32)
        return part(q, zs, me.c, count) + other

    def step(q, _):
        @pl.when(q < n)
        def _():
            for copy in weights(q):
                copy.wait()

            @pl.when(q + depth - 1 < n)
            def _():
                for copy in weights(q + depth - 1):
                    copy.start()

            slot = lax.rem(q, depth)
            for e in range(2):
                block = dot(h_ref[e], wdb[slot, e]).astype(BF16)
                for zs in range(4):
                    o[q, zs, e * size : (e + 1) * size] = block[zs * size : (zs + 1) * size]
            for zs in range(4):
                sd[q, zs * t : (zs + 1) * t] = part(q, zs, 1 - me.c, t).astype(BF16)
            to_partner(q).start()

        @pl.when(jnp.logical_and(q >= 1, q <= n))
        def _():
            r = q - 1
            to_partner(r).wait_recv()

            @pl.when(me.end)
            def _():
                for i, f in enumerate(me.far):
                    sf[r, i, 0:end_rows] = both(r, f, end_rows).astype(BF16)
                    relay(r, i).start()

            sn[r] = both(r, me.near, end_rows).astype(BF16)
            to_near(r).start()

        @pl.when(jnp.logical_and(me.inner, jnp.logical_and(q >= 2, q <= n + 1)))
        def _():
            r = q - 2
            for i, f in enumerate(me.far):
                relay(r, i).wait_recv()
                total = both(r, f, far_rows)
                sf[r, i, 0:end_rows] = (total[:end_rows] + yr[r, i].astype(F32)).astype(BF16)
                if far_rows > end_rows:
                    sf[r, i, end_rows:far_rows] = total[end_rows:].astype(BF16)
                to_far(r, i).start()

        @pl.when(q >= lag)
        def _():
            r = q - lag
            to_near(r).wait_recv()
            to_far(r, 0).wait_recv()
            total = both(r, me.z, t)
            total += dot(qn_ref[:, :end_rows], yn[r])
            total += dot(qf_ref[:, :far_rows], yf[r])
            y_ref[:, pl.ds(pl.multiple_of(r * CW, CW), CW)] = total.astype(BF16)

        return 0

    lax.fori_loop(0, n + lag, step, 0)

    def drain(q, _):
        to_partner(q).wait_send()
        to_near(q).wait_send()

        @pl.when(me.end)
        def _():
            for i in range(2):
                relay(q, i).wait_send()

        @pl.when(me.inner)
        def _():
            for i in range(2):
                to_far(q, i).wait_send()

        return 0

    lax.fori_loop(0, n, drain, 0)


def up_call(x, a, pn, pf, w_gate, w_up, slots, far_rows, end_rows, ident):
    t, d = x.shape
    ff = w_gate.shape[2]
    n, rows = d // CW, 8 * slots
    tiles = ff // CW
    parts = min(4, tiles)
    wide = -(-tiles // parts) * CW
    vmem, hbm = pl.BlockSpec(memory_space=pltpu.VMEM), pl.BlockSpec(memory_space=pl.ANY)
    return pl.pallas_call(
        functools.partial(up_kernel, far_rows, end_rows),
        out_shape=jax.ShapeDtypeStruct((2, rows, ff), BF16),
        in_specs=[vmem] * 4 + [hbm] * 2,
        out_specs=vmem,
        scratch_shapes=[
            pltpu.VMEM((n, 8 * t, CW), BF16),
            pltpu.VMEM((n, end_rows, CW), BF16),
            pltpu.VMEM((n, far_rows, CW), BF16),
            pltpu.VMEM((2, rows, KC), BF16),
            pltpu.VMEM((2, rows, ff), F32),
            pltpu.VMEM((2, rows, ff), F32),
            pltpu.VMEM((parts, KC, wide), BF16),
            pltpu.VMEM((parts, KC, wide), BF16),
            pltpu.SemaphoreType.DMA((parts, 2)),
            pltpu.SemaphoreType.DMA((n, 8)),
            pltpu.SemaphoreType.DMA((n, 8)),
        ],
        compiler_params=pltpu.CompilerParams(collective_id=ident, has_side_effects=True, vmem_limit_bytes=VMEM_BYTES),
        name=f"up_{far_rows}_{end_rows}",
    )(x, a, pn, pf, w_gate, w_up)


def down_call(h, cw, qn, qf, w_down, far_rows, end_rows, ident):
    _, rows, ff = h.shape
    d, t = w_down.shape[2], qn.shape[0]
    n = d // CW
    vmem, hbm = pl.BlockSpec(memory_space=pltpu.VMEM), pl.BlockSpec(memory_space=pl.ANY)
    return pl.pallas_call(
        functools.partial(down_kernel, far_rows, end_rows),
        out_shape=jax.ShapeDtypeStruct((t, d), BF16),
        in_specs=[vmem] * 4 + [hbm],
        out_specs=vmem,
        scratch_shapes=[
            pltpu.VMEM((n, 4, rows // 2, CW), BF16),
            pltpu.VMEM((n, 4 * t, CW), BF16),
            pltpu.VMEM((n, end_rows, CW), BF16),
            pltpu.VMEM((n, far_rows, CW), BF16),
            pltpu.VMEM((n, 2, end_rows, CW), BF16),
            pltpu.VMEM((n, 4 * t, CW), BF16),
            pltpu.VMEM((n, end_rows, CW), BF16),
            pltpu.VMEM((n, 2, far_rows, CW), BF16),
            pltpu.VMEM((3, 2, ff, CW), BF16),
            pltpu.SemaphoreType.DMA((3, 2)),
            pltpu.SemaphoreType.DMA((n, 4)),
            pltpu.SemaphoreType.DMA((n,)),
            pltpu.SemaphoreType.DMA((n,)),
            pltpu.SemaphoreType.DMA((n,)),
            pltpu.SemaphoreType.DMA((n, 2)),
        ],
        compiler_params=pltpu.CompilerParams(collective_id=ident, has_side_effects=True, vmem_limit_bytes=VMEM_BYTES),
        name=f"down_{far_rows}_{end_rows}",
    )(h, cw, qn, qf, w_down)


def route_call(expert, slot, gate, slots, sizes, several):
    t = expert.shape[1]
    vmem = pl.BlockSpec(memory_space=pltpu.VMEM)
    square = jax.ShapeDtypeStruct((t, t), BF16)
    return pl.pallas_call(
        functools.partial(route_kernel, slots, sizes, several),
        out_shape=[
            jax.ShapeDtypeStruct((4, 4 * slots, 2 * t), BF16),
            jax.ShapeDtypeStruct((4, 2 * t, 4 * slots), BF16),
            square,
            square,
            square,
            square,
            jax.ShapeDtypeStruct((8, 128), jnp.int32),
        ],
        in_specs=[vmem] * 3,
        out_specs=[vmem] * 7,
        scratch_shapes=[
            pltpu.VMEM((8, t), F32),
            pltpu.VMEM((8, 8, t), F32),
            pltpu.VMEM((8, 128), F32),
            pltpu.VMEM((3, 8, 128), F32),
            pltpu.SemaphoreType.DMA((7,)),
            pltpu.SemaphoreType.DMA((8,)),
            pltpu.SemaphoreType.DMA((3,)),
            pltpu.SemaphoreType.DMA((3,)),
        ],
        compiler_params=pltpu.CompilerParams(collective_id=0, has_side_effects=True),
        name="route",
    )(expert, slot, gate)


def solution(mesh):
    def body(x, expert, slot, gate, w_gate, w_up, w_down):
        x, expert, slot, gate = x[0, 0], expert[0, 0], slot[0, 0], gate[0, 0]
        t = x.shape[0]
        slots = 5 * t * 2 // (4 * 16)
        sizes = [(160, 112), (192, 144), (t, 4 * slots)]
        a, cw, pn, pf, qn, qf, pick = route_call(expert.T, slot.T, gate.T, slots, sizes, mesh.shape["dp"] > 1)

        def branch(i):
            def run(x, w_gate, w_up, w_down):
                far_rows, end_rows = sizes[i]
                h = up_call(x, a, pn, pf, w_gate, w_up, slots, far_rows, end_rows, 1 + 2 * i)
                return down_call(h, cw, qn, qf, w_down, far_rows, end_rows, 2 + 2 * i)

            return run

        y = lax.switch(pick[0, 0], [branch(i) for i in range(len(sizes))], x, w_gate, w_up, w_down)
        return y[None, None]

    data, weight = P("dp", "ep", None, None), P("ep", None, None)
    return jax.shard_map(
        body,
        mesh=mesh,
        in_specs=(data, data, data, data, weight, weight, weight),
        out_specs=data,
        check_vma=False,
    )
```

```python
import functools

import jax
import jax.numpy as jnp
from jax import lax
from jax.experimental import pallas as pl
from jax.experimental.pallas import tpu as pltpu
from jax.sharding import PartitionSpec as P

MESH = pl.DeviceIdType.MESH
BF16, F32 = jnp.bfloat16, jnp.float32
CW = 256
KC = 512
AHEAD = 3
VMEM_BYTES = 67043328


def dot(a, b):
    return jnp.dot(a, b, preferred_element_type=F32)


def dot_nt(a, b):
    return lax.dot_general(a, b, (((1,), (1,)), ((), ())), preferred_element_type=F32)


class Place:
    def __init__(self):
        self.dp = lax.axis_index("dp")
        self.ep = lax.axis_index("ep")
        self.z = lax.div(self.ep, 2)
        self.c = lax.rem(self.ep, 2)
        half = lax.div(self.z, 2)
        self.near = self.z + 1 - 2 * lax.rem(self.z, 2)
        self.far_inner = 2 - half
        self.far = [2 * (1 - half), 2 * (1 - half) + 1]
        self.inner = jnp.logical_or(self.z == 1, self.z == 2)
        self.end = jnp.logical_or(self.z == 0, self.z == 3)

    def dev(self, z, c):
        return (self.dp, 2 * z + c)

    def greet(self, sem):
        for i in range(1, 8):
            peer = lax.rem(self.ep + i, 8)
            pl.semaphore_signal(sem, inc=1, device_id=(self.dp, peer), device_id_type=MESH)


class Packs:
    def __init__(self, me, every):
        t = every.shape[2]
        self.e = [every[:, 0, :], every[:, 1, :]]
        self.s = [every[:, 2, :], every[:, 3, :]]
        self.g = [every[:, 4, :], every[:, 5, :]]
        self.src = lax.broadcasted_iota(jnp.int32, (8, t), 0)
        zs = self.src // 2
        chip = [jnp.floor(v * 0.25).astype(jnp.int32) for v in self.e]

        def needs(where):
            return jnp.logical_or(chip[0] == where, chip[1] == where)

        self.m_n = needs(zs + 1 - 2 * (zs % 2))
        self.m_a = needs(3 - 3 * (zs // 2))
        self.m_b = jnp.logical_and(needs(2 - zs // 2), jnp.logical_not(self.m_a))

    def order(self, me):
        t = self.src.shape[1]
        self.row = lax.broadcasted_iota(jnp.int32, (t, t), 0)
        self.col = lax.broadcasted_iota(jnp.int32, (t, t), 1)
        before = (self.row < self.col).astype(F32).astype(BF16)

        def count(mask):
            return dot(mask.astype(F32).astype(BF16), before).astype(jnp.int32)

        total_a = jnp.sum(self.m_a.astype(F32), axis=1, keepdims=True).astype(jnp.int32)
        self.pos_n = jnp.where(self.m_n, count(self.m_n), -1)
        self.pos_f = jnp.where(self.m_a, count(self.m_a), jnp.where(self.m_b, total_a + count(self.m_b), -1))

    def own(self, me, pos):
        return jnp.sum(jnp.where(self.src == me.ep, pos, 0).astype(F32), axis=0, keepdims=True)

    def packers(self, me, pn_ref, pf_ref):
        for pos, p_ref in ((self.pos_n, pn_ref), (self.pos_f, pf_ref)):
            p_ref[...] = (self.row == self.own(me, pos).astype(jnp.int32)).astype(F32).astype(BF16)

    def matrices(self, me, slots, a_ref, cw_ref, qn_ref, qf_ref):
        t = self.src.shape[1]
        row, col, src = self.row, self.col, self.src
        zs, cs = src // 2, src % 2
        lane = lax.broadcasted_iota(jnp.int32, (8, t), 1)
        pos = jnp.where(zs == me.z, lane, jnp.where(zs == me.near, self.pos_n, self.pos_f))
        codes = []
        for j in range(2):
            local = self.e[j].astype(jnp.int32) - 2 * me.ep
            hit = jnp.logical_and(local >= 0, local < 2)
            code = local * (2 * slots) + cs * slots + self.s[j].astype(jnp.int32) + 1
            codes.append(jnp.where(hit, code, 0).astype(F32))
        table = jnp.concatenate(codes + self.g, axis=0).astype(BF16)
        slot_row = lax.broadcasted_iota(jnp.int32, (4 * slots, t), 0) + 1
        slot_col = lax.broadcasted_iota(jnp.int32, (t, 4 * slots), 1) + 1
        for k in range(8):
            perm = (row == pos[k : k + 1]).astype(F32).astype(BF16)
            by_row = dot_nt(table, perm)
            by_col = dot_nt(perm, table)
            r0 = by_row[k : k + 1].astype(jnp.int32)
            r1 = by_row[8 + k : 9 + k].astype(jnp.int32)
            c0 = by_col[:, k : k + 1].astype(jnp.int32)
            c1 = by_col[:, 8 + k : 9 + k].astype(jnp.int32)
            g0, g1 = by_col[:, 16 + k : 17 + k], by_col[:, 24 + k : 25 + k]
            hit = jnp.logical_or(slot_row == r0, slot_row == r1)
            place = slice((k % 2) * t, (k % 2 + 1) * t)
            a_ref[k // 2, :, place] = hit.astype(F32).astype(BF16)
            weight = jnp.where(slot_col == c0, g0, 0.0) + jnp.where(slot_col == c1, g1, 0.0)
            cw_ref[k // 2, place, :] = weight.astype(BF16)
        eye = (row == col).astype(F32).astype(BF16)
        for pos_x, q_ref in ((self.pos_n, qn_ref), (self.pos_f, qf_ref)):
            order = jnp.broadcast_to(self.own(me, pos_x), (8, t)).astype(BF16)
            column = dot_nt(eye, order)[:, 0:1]
            q_ref[...] = (col == column.astype(jnp.int32)).astype(F32).astype(BF16)


def route_kernel(slots, sizes, several, expert_ref, slot_ref, gate_ref, every, pick_ref, mine, top, tops, send_sem, recv_sem, top_send, top_recv):
    me = Place()
    t = expert_ref.shape[1]
    barrier = pltpu.get_barrier_semaphore()
    peers = [(me.dp, lax.rem(me.ep + i, 8)) for i in range(1, 8)]
    groups = [(lax.rem(me.dp + i, 4), me.ep) for i in range(1, 4)]
    if not several:
        groups = []
    for peer in peers + groups:
        pl.semaphore_signal(barrier, inc=1, device_id=peer, device_id_type=MESH)
    slot = slot_ref[...]
    mine[0:2] = jnp.where(slot < slots, expert_ref[...], -1).astype(F32)
    mine[2:4] = jnp.minimum(slot, slots).astype(F32)
    mine[4:6] = gate_ref[...]
    mine[6:8] = jnp.zeros((2, t), F32)
    pl.semaphore_wait(barrier, len(peers) + len(groups))

    def table_to(i):
        return pltpu.make_async_remote_copy(
            src_ref=mine,
            dst_ref=every.at[me.ep],
            send_sem=send_sem.at[i],
            recv_sem=recv_sem.at[me.ep],
            device_id=peers[i],
            device_id_type=MESH,
        )

    def table_from(i):
        source = lax.rem(me.ep + 8 - i, 8)
        return pltpu.make_async_remote_copy(
            src_ref=mine,
            dst_ref=every.at[source],
            send_sem=send_sem.at[0],
            recv_sem=recv_sem.at[source],
            device_id=peers[0],
            device_id_type=MESH,
        )

    for i in range(7):
        table_to(i).start()
    every[me.ep] = mine[...]
    for i in range(1, 8):
        table_from(i).wait_recv()

    packs = Packs(me, every)
    def most(mask):
        return jnp.max(jnp.sum(mask.astype(F32), axis=1, keepdims=True), axis=0, keepdims=True)

    far_top = most(jnp.logical_or(packs.m_a, packs.m_b))
    end_top = jnp.maximum(most(packs.m_a), most(packs.m_n))
    which = lax.broadcasted_iota(jnp.int32, (8, 128), 0)
    top[...] = jnp.where(which == 0, far_top, end_top)

    def top_copy(i, slot):
        return pltpu.make_async_remote_copy(
            src_ref=top,
            dst_ref=tops.at[slot],
            send_sem=top_send.at[i],
            recv_sem=top_recv.at[slot],
            device_id=groups[i],
            device_id_type=MESH,
        )

    for i in range(len(groups)):
        top_copy(i, i).start()

    limit = top[...]
    for i in range(len(groups)):
        top_copy(i, i).wait_recv()
        limit = jnp.maximum(limit, tops[i])
    far_max, end_max = limit[0:1], limit[1:2]
    pick = jnp.full((1, 128), len(sizes) - 1, jnp.int32)
    for i, (far_rows, end_rows) in reversed(list(enumerate(sizes[:-1]))):
        pick = jnp.where(jnp.logical_and(far_max <= far_rows, end_max <= end_rows), i, pick)
    pick_ref[0, 0] = jnp.max(pick)
    for i in range(7):
        table_to(i).wait_send()
    for i in range(len(groups)):
        top_copy(i, i).wait_send()


def up_kernel(unroll, slots, far_rows, end_rows, x_ref, every, a_ref, cw_ref, pn_ref, pf_ref, qn_ref, qf_ref, wg_hbm, wu_hbm, h_ref, xall, sn, sf, zbuf, gacc, uacc, wgb, wub, wsem, send_sem, recv_sem):
    me = Place()
    t, d = x_ref.shape
    ff = wg_hbm.shape[2]
    rows = zbuf.shape[1]
    n, nk = d // CW, d // KC
    tiles = ff // CW
    parts = wgb.shape[0]
    sizes = [tiles // parts + (i < tiles % parts) for i in range(parts)]
    starts = [sum(sizes[:i]) for i in range(parts)]

    def weights(u, p):
        e, k = lax.rem(u, 2), lax.div(u, 2)
        for i, (hbm, buf) in enumerate(((wg_hbm, wgb), (wu_hbm, wub))):
            yield pltpu.make_async_copy(
                hbm.at[e, pl.ds(pl.multiple_of(k * KC, KC), KC), pl.ds(starts[p] * CW, sizes[p] * CW)],
                buf.at[p, :, pl.ds(0, sizes[p] * CW)],
                wsem.at[p, i],
            )

    barrier = pltpu.get_barrier_semaphore()
    me.greet(barrier)
    for p in range(parts):
        for copy in weights(0, p):
            copy.start()

    def cell(j, slot, count):
        return xall.at[j, pl.ds(pl.multiple_of(slot * t, t), count)]

    def remote(j, kind, src, slot, count, to):
        return pltpu.make_async_remote_copy(
            src_ref=src,
            dst_ref=cell(j, slot, count),
            send_sem=send_sem.at[j, kind],
            recv_sem=recv_sem.at[j, slot],
            device_id=to,
            device_id_type=MESH,
        )

    partner, nearby = me.dev(me.z, 1 - me.c), me.dev(me.near, me.c)
    own, near_slot = me.ep, 2 * me.near + me.c
    far_slots = [2 * f + me.c for f in me.far]

    def sends(j):
        cols = pl.ds(pl.multiple_of(j * CW, CW), CW)
        yield remote(j, 2, sf.at[j], own, far_rows, me.dev(me.far_inner, me.c))
        yield remote(j, 1, sn.at[j], own, end_rows, nearby)
        yield remote(j, 0, x_ref.at[:, cols], own, t, partner)

    def forward(j, kind, slot, count, to):
        return remote(j, kind, cell(j, slot, count), slot, count, to)

    def arrived(j, slot, count):
        forward(j, 0, slot, count, partner).wait_recv()

    def pack(j, _):
        cols = pl.ds(pl.multiple_of(j * CW, CW), CW)
        block = x_ref[:, cols]
        sf[j] = dot(pf_ref[:far_rows], block).astype(BF16)
        sn[j] = dot(pn_ref[:end_rows], block).astype(BF16)
        xall[j, pl.ds(pl.multiple_of(own * t, t), t)] = block
        return 0

    def send(j):
        for copy in sends(j):
            copy.start()

    def clear(j, _):
        def zero(slot, start, stop):
            if stop > start:
                xall[j, pl.ds(pl.multiple_of(slot * t + start, 16), stop - start)] = jnp.zeros((stop - start, CW), BF16)

        for i in range(2):
            zero(2 * me.near + i, end_rows, t)
            for f in me.far:
                zero(2 * f + i, far_rows, t)

        @pl.when(me.end)
        def _():
            for i in range(2):
                for f in me.far:
                    zero(2 * f + i, end_rows, far_rows)

        return 0

    packs = Packs(me, every)
    packs.order(me)
    packs.packers(me, pn_ref, pf_ref)
    for j in range(AHEAD):
        pack(j, 0)
        if j == 0:
            pl.semaphore_wait(barrier, 7)
        send(j)
    lax.fori_loop(AHEAD, n, pack, 0)
    lax.fori_loop(0, n, clear, 0)

    def clear_sums(i, _):
        cols = pl.ds(pl.multiple_of(i * CW, CW), CW)
        for e in range(2):
            gacc[e, :, cols] = jnp.zeros((rows, CW), F32)
            uacc[e, :, cols] = jnp.zeros((rows, CW), F32)
        return 0

    lax.fori_loop(0, tiles, clear_sums, 0)

    def gather(k):
        for i in range(2):
            j = 2 * k + i
            arrived(j, 2 * me.z + 1 - me.c, t)
            arrived(j, 2 * me.near + 1 - me.c, end_rows)
            for f in me.far:

                @pl.when(me.inner)
                def _():
                    arrived(j, 2 * f + 1 - me.c, far_rows)

                @pl.when(me.end)
                def _():
                    arrived(j, 2 * f + 1 - me.c, end_rows)

            for zs in range(4):
                block = dot(a_ref[zs], xall[j, zs * 2 * t : (zs + 1) * 2 * t]).astype(BF16)
                size = rows // 4
                for e in range(2):
                    zbuf[e, zs * size : (zs + 1) * size, i * CW : (i + 1) * CW] = block[e * size : (e + 1) * size]

    def unit(u):
        e, k = lax.rem(u, 2), lax.div(u, 2)

        @pl.when(e == 0)
        def _():
            gather(k)

        def tiles_of(p, last):
            if p % 2 == 0:
                for r in range(p, min(parts, p + 2)):
                    for copy in weights(u, r):
                        copy.wait()
            def tile(i, _):
                here = pl.ds(pl.multiple_of(i * CW, CW), CW)
                cols = pl.ds(pl.multiple_of((starts[p] + i) * CW, CW), CW)
                z = zbuf[e]
                gate = gacc[e, :, cols] + dot(z, wgb[p, :, here])
                up = uacc[e, :, cols] + dot(z, wub[p, :, here])
                if last:
                    h_ref[e, :, cols] = (gate * jax.nn.sigmoid(gate) * up).astype(BF16)
                else:
                    gacc[e, :, cols] = gate
                    uacc[e, :, cols] = up
                return 0

            lax.fori_loop(0, sizes[p], tile, 0, unroll=unroll)

            def start():
                for copy in weights(u + 1, p):
                    copy.start()

            if last:
                pl.when(u + 1 < 2 * nk)(start)
            else:
                start()

        @pl.when(k < nk - 1)
        def _():
            for p in range(parts):
                tiles_of(p, False)

        @pl.when(k == nk - 1)
        def _():
            for p in range(parts):
                tiles_of(p, True)

    def relay(j):
        @pl.when(j + AHEAD < n)
        def _():
            send(j + AHEAD)

        @pl.when(j < n)
        def _():
            @pl.when(me.inner)
            def _():
                for i, slot in enumerate(far_slots):
                    arrived(j, slot, far_rows)
                    forward(j, 6 + i, slot, end_rows, nearby).start()
                    forward(j, 4 + i, slot, far_rows, partner).start()

            arrived(j, near_slot, end_rows)
            forward(j, 3, near_slot, end_rows, partner).start()

        @pl.when(jnp.logical_and(me.end, jnp.logical_and(j >= 1, j <= n)))
        def _():
            for i, slot in enumerate(far_slots):
                arrived(j - 1, slot, end_rows)
                forward(j - 1, 4 + i, slot, end_rows, partner).start()

    def step(j, _):
        relay(j)

        @pl.when(j >= 3)
        def _():
            unit(j - 3)

        return 0

    relay(jnp.int32(0))
    packs.matrices(me, slots, a_ref, cw_ref, qn_ref, qf_ref)
    lax.fori_loop(1, n + 3, step, 0)

    def drain(j, _):
        for copy in sends(j):
            copy.wait_send()
        forward(j, 3, near_slot, end_rows, partner).wait_send()

        @pl.when(me.inner)
        def _():
            for i, slot in enumerate(far_slots):
                forward(j, 6 + i, slot, end_rows, nearby).wait_send()
                forward(j, 4 + i, slot, far_rows, partner).wait_send()

        @pl.when(me.end)
        def _():
            for i, slot in enumerate(far_slots):
                forward(j, 4 + i, slot, end_rows, partner).wait_send()

        return 0

    lax.fori_loop(0, n, drain, 0)


def down_kernel(far_rows, end_rows, h_ref, cw_ref, qn_ref, qf_ref, wd_hbm, y_hbm, y_ref, y_sem, o, yd, yn, yf, yr, sd, sn, sf, wdb, wsem, send_sem, dsem, nsem, fsem, rsem, ready):
    me = Place()
    t, d = y_ref.shape
    ff = wd_hbm.shape[1]
    rows = h_ref.shape[1]
    size = rows // 4
    n = d // CW
    depth = wdb.shape[0]
    lag = 5

    def weights(q):
        cols = pl.ds(pl.multiple_of(q * CW, CW), CW)
        slot = lax.rem(q, depth)
        for e in range(2):
            yield pltpu.make_async_copy(wd_hbm.at[e, :, cols], wdb.at[slot, e], wsem.at[slot, e])

    me.greet(ready)
    for q in range(depth - 1):
        for copy in weights(q):
            copy.start()

    partner, nearby = me.dev(me.z, 1 - me.c), me.dev(me.near, me.c)

    def remote(q, kind, src, dst, recv, to):
        return pltpu.make_async_remote_copy(
            src_ref=src, dst_ref=dst, send_sem=send_sem.at[q, kind], recv_sem=recv, device_id=to, device_id_type=MESH
        )

    def to_partner(q):
        return remote(q, 0, sd.at[q], yd.at[q], dsem.at[q], partner)

    def to_near(q):
        return remote(q, 1, sn.at[q], yn.at[q], nsem.at[q], nearby)

    def relay(q, i):
        return remote(q, 2 + i, sf.at[q, i, pl.ds(0, end_rows)], yr.at[q, i], rsem.at[q, i], nearby)

    def to_far(q, i):
        return remote(q, 2 + i, sf.at[q, i], yf.at[q], fsem.at[q], me.dev(me.far[i], me.c))

    def result(q):
        cols = pl.ds(pl.multiple_of(q * CW, CW), CW)
        return pltpu.make_async_copy(y_ref.at[:, cols], y_hbm.at[:, cols], y_sem.at[q])

    def part(q, zs, c, count):
        return dot(cw_ref[zs, pl.ds(pl.multiple_of(c * t, t), count), :], o[q, zs])

    def both(q, zs, count):
        other = yd[q, pl.ds(pl.multiple_of(zs * t, t), count)].astype(F32)
        return part(q, zs, me.c, count) + other

    def step(q, _):
        @pl.when(q < n)
        def _():
            for copy in weights(q):
                copy.wait()

            @pl.when(q + depth - 1 < n)
            def _():
                for copy in weights(q + depth - 1):
                    copy.start()

            slot = lax.rem(q, depth)
            for e in range(2):
                block = dot(h_ref[e], wdb[slot, e]).astype(BF16)
                for zs in range(4):
                    o[q, zs, e * size : (e + 1) * size] = block[zs * size : (zs + 1) * size]
            for zs in range(4):
                sd[q, zs * t : (zs + 1) * t] = part(q, zs, 1 - me.c, t).astype(BF16)

            @pl.when(q == 0)
            def _():
                pl.semaphore_wait(ready, 7)

            to_partner(q).start()

        @pl.when(jnp.logical_and(q >= 1, q <= n))
        def _():
            r = q - 1
            to_partner(r).wait_recv()

            @pl.when(me.end)
            def _():
                for i, f in enumerate(me.far):
                    sf[r, i, 0:end_rows] = both(r, f, end_rows).astype(BF16)
                    relay(r, i).start()

            sn[r] = both(r, me.near, end_rows).astype(BF16)
            to_near(r).start()

        @pl.when(jnp.logical_and(me.inner, jnp.logical_and(q >= 2, q <= n + 1)))
        def _():
            r = q - 2
            for i, f in enumerate(me.far):
                relay(r, i).wait_recv()
                total = both(r, f, far_rows)
                sf[r, i, 0:end_rows] = (total[:end_rows] + yr[r, i].astype(F32)).astype(BF16)
                if far_rows > end_rows:
                    sf[r, i, end_rows:far_rows] = total[end_rows:].astype(BF16)
                to_far(r, i).start()

        @pl.when(q >= lag)
        def _():
            r = q - lag
            to_near(r).wait_recv()
            to_far(r, 0).wait_recv()
            total = both(r, me.z, t)
            total += dot(qn_ref[:, :end_rows], yn[r])
            total += dot(qf_ref[:, :far_rows], yf[r])
            y_ref[:, pl.ds(pl.multiple_of(r * CW, CW), CW)] = total.astype(BF16)
            result(r).start()

        return 0

    lax.fori_loop(0, n + lag, step, 0)

    def drain(q, _):
        result(q).wait()
        to_partner(q).wait_send()
        to_near(q).wait_send()

        @pl.when(me.end)
        def _():
            for i in range(2):
                relay(q, i).wait_send()

        @pl.when(me.inner)
        def _():
            for i in range(2):
                to_far(q, i).wait_send()

        return 0

    lax.fori_loop(0, n, drain, 0)


def moe_kernel(unroll, slots, far_rows, end_rows, x, every, wg, wu, wd, y, h, a, cw, pn, pf, qn, qf, ready, up_wsem, up_send, up_recv, down_wsem, down_send, dsem, nsem, fsem, rsem, y_sem):
    t, d = x.shape
    n, rows, ff = d // CW, h.shape[1], h.shape[2]
    parts = up_wsem.shape[0]
    wide = -(-(ff // CW) // parts) * CW

    def first(xall, sn, sf, zbuf, gacc, uacc, wgb, wub):
        up_kernel(unroll, slots, far_rows, end_rows, x, every, a, cw, pn, pf, qn, qf, wg, wu, h, xall, sn, sf, zbuf, gacc, uacc, wgb, wub, up_wsem, up_send, up_recv)

    pl.run_scoped(
        first,
        pltpu.VMEM((n, 8 * t, CW), BF16),
        pltpu.VMEM((n, end_rows, CW), BF16),
        pltpu.VMEM((n, far_rows, CW), BF16),
        pltpu.VMEM((2, rows, KC), BF16),
        pltpu.VMEM((2, rows, ff), F32),
        pltpu.VMEM((2, rows, ff), F32),
        pltpu.VMEM((parts, KC, wide), BF16),
        pltpu.VMEM((parts, KC, wide), BF16),
    )

    def second(y_stage, o, yd, yn, yf, yr, sd, sn, sf, wdb):
        down_kernel(far_rows, end_rows, h, cw, qn, qf, wd, y, y_stage, y_sem, o, yd, yn, yf, yr, sd, sn, sf, wdb, down_wsem, down_send, dsem, nsem, fsem, rsem, ready)

    pl.run_scoped(
        second,
        pltpu.VMEM((t, d), BF16),
        pltpu.VMEM((n, 4, rows // 2, CW), BF16),
        pltpu.VMEM((n, 4 * t, CW), BF16),
        pltpu.VMEM((n, end_rows, CW), BF16),
        pltpu.VMEM((n, far_rows, CW), BF16),
        pltpu.VMEM((n, 2, end_rows, CW), BF16),
        pltpu.VMEM((n, 4 * t, CW), BF16),
        pltpu.VMEM((n, end_rows, CW), BF16),
        pltpu.VMEM((n, 2, far_rows, CW), BF16),
        pltpu.VMEM((down_wsem.shape[0], 2, ff, CW), BF16),
    )


def moe_call(x, every, w_gate, w_up, w_down, slots, far_rows, end_rows, unroll, ident):
    t, d = x.shape
    ff = w_gate.shape[2]
    n, rows = d // CW, 8 * slots
    parts = min(4, ff // CW)
    vmem, hbm = pl.BlockSpec(memory_space=pltpu.VMEM), pl.BlockSpec(memory_space=pl.ANY)
    return pl.pallas_call(
        functools.partial(moe_kernel, unroll, slots, far_rows, end_rows),
        out_shape=jax.ShapeDtypeStruct((t, d), BF16),
        in_specs=[vmem] * 2 + [hbm] * 3,
        out_specs=hbm,
        scratch_shapes=[
            pltpu.VMEM((2, rows, ff), BF16),
            pltpu.VMEM((4, 4 * slots, 2 * t), BF16),
            pltpu.VMEM((4, 2 * t, 4 * slots), BF16),
            pltpu.VMEM((t, t), BF16),
            pltpu.VMEM((t, t), BF16),
            pltpu.VMEM((t, t), BF16),
            pltpu.VMEM((t, t), BF16),
            pltpu.SemaphoreType.REGULAR,
            pltpu.SemaphoreType.DMA((parts, 2)),
            pltpu.SemaphoreType.DMA((n, 8)),
            pltpu.SemaphoreType.DMA((n, 8)),
            pltpu.SemaphoreType.DMA((3, 2)),
            pltpu.SemaphoreType.DMA((n, 4)),
            pltpu.SemaphoreType.DMA((n,)),
            pltpu.SemaphoreType.DMA((n,)),
            pltpu.SemaphoreType.DMA((n,)),
            pltpu.SemaphoreType.DMA((n, 2)),
            pltpu.SemaphoreType.DMA((n,)),
        ],
        compiler_params=pltpu.CompilerParams(collective_id=ident, has_side_effects=True, vmem_limit_bytes=VMEM_BYTES),
        name=f"moe_{far_rows}_{end_rows}",
    )(x, every, w_gate, w_up, w_down)


def route_call(expert, slot, gate, slots, sizes, several):
    t = expert.shape[1]
    vmem = pl.BlockSpec(memory_space=pltpu.VMEM)
    return pl.pallas_call(
        functools.partial(route_kernel, slots, sizes, several),
        out_shape=[jax.ShapeDtypeStruct((8, 8, t), F32), jax.ShapeDtypeStruct((1, 1), jnp.int32)],
        in_specs=[vmem] * 3,
        out_specs=[vmem, pl.BlockSpec(memory_space=pltpu.SMEM)],
        scratch_shapes=[
            pltpu.VMEM((8, t), F32),
            pltpu.VMEM((8, 128), F32),
            pltpu.VMEM((3, 8, 128), F32),
            pltpu.SemaphoreType.DMA((7,)),
            pltpu.SemaphoreType.DMA((8,)),
            pltpu.SemaphoreType.DMA((3,)),
            pltpu.SemaphoreType.DMA((3,)),
        ],
        compiler_params=pltpu.CompilerParams(collective_id=0, has_side_effects=True),
        name="route",
    )(expert, slot, gate)


def solution(mesh):
    def body(x, expert, slot, gate, w_gate, w_up, w_down):
        x, expert, slot, gate = x[0, 0], expert[0, 0], slot[0, 0], gate[0, 0]
        t = x.shape[0]
        slots = 5 * t * 2 // (4 * 16)
        sizes = [(160, 112), (192, 144), (t, 4 * slots)]
        every, pick = route_call(expert.T, slot.T, gate.T, slots, sizes, mesh.shape["dp"] > 1)

        def branch(i):
            def run(x, w_gate, w_up, w_down):
                far_rows, end_rows = sizes[i]
                return moe_call(x, every, w_gate, w_up, w_down, slots, far_rows, end_rows, i == 0, 1 + i)

            return run

        y = lax.switch(pick[0, 0], [branch(i) for i in range(len(sizes))], x, w_gate, w_up, w_down)
        return y[None, None]

    data, weight = P("dp", "ep", None, None), P("ep", None, None)
    return jax.shard_map(
        body,
        mesh=mesh,
        in_specs=(data, data, data, data, weight, weight, weight),
        out_specs=data,
        check_vma=False,
    )
```

```python
import functools

import jax
import jax.numpy as jnp
from jax import lax
from jax.experimental import pallas as pl
from jax.experimental.pallas import tpu as pltpu
from jax.sharding import PartitionSpec as P

MESH = pl.DeviceIdType.MESH
BF16, F32 = jnp.bfloat16, jnp.float32
CW = 256
KC = 512
AHEAD = 3
VMEM_BYTES = 67043328


def dot(a, b):
    return jnp.dot(a, b, preferred_element_type=F32)


def dot_nt(a, b):
    return lax.dot_general(a, b, (((1,), (1,)), ((), ())), preferred_element_type=F32)


class Place:
    def __init__(self):
        self.dp = lax.axis_index("dp")
        self.ep = lax.axis_index("ep")
        self.z = lax.div(self.ep, 2)
        self.c = lax.rem(self.ep, 2)
        half = lax.div(self.z, 2)
        self.near = self.z + 1 - 2 * lax.rem(self.z, 2)
        self.far_inner = 2 - half
        self.far = [2 * (1 - half), 2 * (1 - half) + 1]
        self.inner = jnp.logical_or(self.z == 1, self.z == 2)
        self.end = jnp.logical_or(self.z == 0, self.z == 3)

    def dev(self, z, c):
        return (self.dp, 2 * z + c)

    def greet(self, sem):
        for i in range(1, 8):
            peer = lax.rem(self.ep + i, 8)
            pl.semaphore_signal(sem, inc=1, device_id=(self.dp, peer), device_id_type=MESH)


class Packs:
    def __init__(self, me, every):
        t = every.shape[2]
        self.e = [every[:, 0, :], every[:, 1, :]]
        self.s = [every[:, 2, :], every[:, 3, :]]
        self.g = [every[:, 4, :], every[:, 5, :]]
        self.src = lax.broadcasted_iota(jnp.int32, (8, t), 0)
        zs = self.src // 2
        chip = [jnp.floor(v * 0.25).astype(jnp.int32) for v in self.e]

        def needs(where):
            return jnp.logical_or(chip[0] == where, chip[1] == where)

        self.m_n = needs(zs + 1 - 2 * (zs % 2))
        self.m_a = needs(3 - 3 * (zs // 2))
        self.m_b = jnp.logical_and(needs(2 - zs // 2), jnp.logical_not(self.m_a))

    def order(self, me):
        t = self.src.shape[1]
        self.row = lax.broadcasted_iota(jnp.int32, (t, t), 0)
        self.col = lax.broadcasted_iota(jnp.int32, (t, t), 1)
        before = (self.row < self.col).astype(F32).astype(BF16)

        def count(mask):
            return dot(mask.astype(F32).astype(BF16), before).astype(jnp.int32)

        total_a = jnp.sum(self.m_a.astype(F32), axis=1, keepdims=True).astype(jnp.int32)
        self.pos_n = jnp.where(self.m_n, count(self.m_n), -1)
        self.pos_f = jnp.where(self.m_a, count(self.m_a), jnp.where(self.m_b, total_a + count(self.m_b), -1))

    def own(self, me, pos):
        return jnp.sum(jnp.where(self.src == me.ep, pos, 0).astype(F32), axis=0, keepdims=True)

    def packers(self, me, pn_ref, pf_ref):
        for pos, p_ref in ((self.pos_n, pn_ref), (self.pos_f, pf_ref)):
            p_ref[...] = (self.row == self.own(me, pos).astype(jnp.int32)).astype(F32).astype(BF16)

    def matrices(self, me, slots, a_ref, cw_ref, qn_ref, qf_ref):
        t = self.src.shape[1]
        row, col, src = self.row, self.col, self.src
        zs, cs = src // 2, src % 2
        lane = lax.broadcasted_iota(jnp.int32, (8, t), 1)
        pos = jnp.where(zs == me.z, lane, jnp.where(zs == me.near, self.pos_n, self.pos_f))
        codes = []
        for j in range(2):
            local = self.e[j].astype(jnp.int32) - 2 * me.ep
            hit = jnp.logical_and(local >= 0, local < 2)
            code = local * (2 * slots) + cs * slots + self.s[j].astype(jnp.int32) + 1
            codes.append(jnp.where(hit, code, 0).astype(F32))
        table = jnp.concatenate(codes + self.g, axis=0).astype(BF16)
        slot_row = lax.broadcasted_iota(jnp.int32, (4 * slots, t), 0) + 1
        slot_col = lax.broadcasted_iota(jnp.int32, (t, 4 * slots), 1) + 1
        for k in range(8):
            perm = (row == pos[k : k + 1]).astype(F32).astype(BF16)
            by_row = dot_nt(table, perm)
            by_col = dot_nt(perm, table)
            r0 = by_row[k : k + 1].astype(jnp.int32)
            r1 = by_row[8 + k : 9 + k].astype(jnp.int32)
            c0 = by_col[:, k : k + 1].astype(jnp.int32)
            c1 = by_col[:, 8 + k : 9 + k].astype(jnp.int32)
            g0, g1 = by_col[:, 16 + k : 17 + k], by_col[:, 24 + k : 25 + k]
            hit = jnp.logical_or(slot_row == r0, slot_row == r1)
            place = slice((k % 2) * t, (k % 2 + 1) * t)
            a_ref[k // 2, :, place] = hit.astype(F32).astype(BF16)
            weight = jnp.where(slot_col == c0, g0, 0.0) + jnp.where(slot_col == c1, g1, 0.0)
            cw_ref[k // 2, place, :] = weight.astype(BF16)
        eye = (row == col).astype(F32).astype(BF16)
        for pos_x, q_ref in ((self.pos_n, qn_ref), (self.pos_f, qf_ref)):
            order = jnp.broadcast_to(self.own(me, pos_x), (8, t)).astype(BF16)
            column = dot_nt(eye, order)[:, 0:1]
            q_ref[...] = (col == column.astype(jnp.int32)).astype(F32).astype(BF16)


def route_kernel(slots, sizes, several, expert_ref, slot_ref, gate_ref, every, pick_ref, mine, top, tops, send_sem, recv_sem, top_send, top_recv):
    me = Place()
    t = expert_ref.shape[1]
    barrier = pltpu.get_barrier_semaphore()
    peers = [(me.dp, lax.rem(me.ep + i, 8)) for i in range(1, 8)]
    groups = [(lax.rem(me.dp + i, 4), me.ep) for i in range(1, 4)]
    if not several:
        groups = []
    for peer in peers + groups:
        pl.semaphore_signal(barrier, inc=1, device_id=peer, device_id_type=MESH)
    slot = slot_ref[...]
    mine[0:2] = jnp.where(slot < slots, expert_ref[...], -1).astype(F32)
    mine[2:4] = jnp.minimum(slot, slots).astype(F32)
    mine[4:6] = gate_ref[...]
    mine[6:8] = jnp.zeros((2, t), F32)
    pl.semaphore_wait(barrier, len(peers) + len(groups))

    def table_to(i):
        return pltpu.make_async_remote_copy(
            src_ref=mine,
            dst_ref=every.at[me.ep],
            send_sem=send_sem.at[i],
            recv_sem=recv_sem.at[me.ep],
            device_id=peers[i],
            device_id_type=MESH,
        )

    def table_from(i):
        source = lax.rem(me.ep + 8 - i, 8)
        return pltpu.make_async_remote_copy(
            src_ref=mine,
            dst_ref=every.at[source],
            send_sem=send_sem.at[0],
            recv_sem=recv_sem.at[source],
            device_id=peers[0],
            device_id_type=MESH,
        )

    for i in range(7):
        table_to(i).start()
    every[me.ep] = mine[...]
    for i in range(1, 8):
        table_from(i).wait_recv()

    packs = Packs(me, every)
    def most(mask):
        return jnp.max(jnp.sum(mask.astype(F32), axis=1, keepdims=True), axis=0, keepdims=True)

    far_top = most(jnp.logical_or(packs.m_a, packs.m_b))
    end_top = jnp.maximum(most(packs.m_a), most(packs.m_n))
    which = lax.broadcasted_iota(jnp.int32, (8, 128), 0)
    top[...] = jnp.where(which == 0, far_top, end_top)

    def top_copy(i, slot):
        return pltpu.make_async_remote_copy(
            src_ref=top,
            dst_ref=tops.at[slot],
            send_sem=top_send.at[i],
            recv_sem=top_recv.at[slot],
            device_id=groups[i],
            device_id_type=MESH,
        )

    for i in range(len(groups)):
        top_copy(i, i).start()

    limit = top[...]
    for i in range(len(groups)):
        top_copy(i, i).wait_recv()
        limit = jnp.maximum(limit, tops[i])
    far_max, end_max = limit[0:1], limit[1:2]
    pick = jnp.full((1, 128), len(sizes) - 1, jnp.int32)
    for i, (far_rows, end_rows) in reversed(list(enumerate(sizes[:-1]))):
        pick = jnp.where(jnp.logical_and(far_max <= far_rows, end_max <= end_rows), i, pick)
    pick_ref[0, 0] = jnp.max(pick)
    for i in range(7):
        table_to(i).wait_send()
    for i in range(len(groups)):
        top_copy(i, i).wait_send()


def up_kernel(unroll, slots, far_rows, end_rows, x_ref, every, a_ref, cw_ref, pn_ref, pf_ref, qn_ref, qf_ref, wg_hbm, wu_hbm, h_ref, xall, sn, sf, zbuf, gacc, uacc, wgb, wub, wsem, send_sem, recv_sem):
    me = Place()
    t, d = x_ref.shape
    ff = wg_hbm.shape[2]
    rows = zbuf.shape[1]
    n, nk = d // CW, d // KC
    tiles = ff // CW
    parts = wgb.shape[0]
    sizes = [tiles // parts + (i < tiles % parts) for i in range(parts)]
    starts = [sum(sizes[:i]) for i in range(parts)]

    def weights(u, p):
        e, k = lax.rem(u, 2), lax.div(u, 2)
        for i, (hbm, buf) in enumerate(((wg_hbm, wgb), (wu_hbm, wub))):
            yield pltpu.make_async_copy(
                hbm.at[e, pl.ds(pl.multiple_of(k * KC, KC), KC), pl.ds(starts[p] * CW, sizes[p] * CW)],
                buf.at[p, :, pl.ds(0, sizes[p] * CW)],
                wsem.at[p, i],
            )

    barrier = pltpu.get_barrier_semaphore()
    me.greet(barrier)
    for p in range(parts):
        for copy in weights(0, p):
            copy.start()

    def cell(j, slot, count):
        return xall.at[j, pl.ds(pl.multiple_of(slot * t, t), count)]

    def remote(j, kind, src, slot, count, to):
        return pltpu.make_async_remote_copy(
            src_ref=src,
            dst_ref=cell(j, slot, count),
            send_sem=send_sem.at[j, kind],
            recv_sem=recv_sem.at[j, slot],
            device_id=to,
            device_id_type=MESH,
        )

    partner, nearby = me.dev(me.z, 1 - me.c), me.dev(me.near, me.c)
    own, near_slot = me.ep, 2 * me.near + me.c
    far_slots = [2 * f + me.c for f in me.far]

    def sends(j):
        cols = pl.ds(pl.multiple_of(j * CW, CW), CW)
        yield remote(j, 2, sf.at[j], own, far_rows, me.dev(me.far_inner, me.c))
        yield remote(j, 1, sn.at[j], own, end_rows, nearby)
        yield remote(j, 0, x_ref.at[:, cols], own, t, partner)

    def forward(j, kind, slot, count, to):
        return remote(j, kind, cell(j, slot, count), slot, count, to)

    def arrived(j, slot, count):
        forward(j, 0, slot, count, partner).wait_recv()

    def pack(j, _):
        cols = pl.ds(pl.multiple_of(j * CW, CW), CW)
        block = x_ref[:, cols]
        sf[j] = dot(pf_ref[:far_rows], block).astype(BF16)
        sn[j] = dot(pn_ref[:end_rows], block).astype(BF16)
        xall[j, pl.ds(pl.multiple_of(own * t, t), t)] = block
        return 0

    def send(j):
        for copy in sends(j):
            copy.start()

    def clear(j, _):
        def zero(slot, start, stop):
            if stop > start:
                xall[j, pl.ds(pl.multiple_of(slot * t + start, 16), stop - start)] = jnp.zeros((stop - start, CW), BF16)

        for i in range(2):
            zero(2 * me.near + i, end_rows, t)
            for f in me.far:
                zero(2 * f + i, far_rows, t)

        @pl.when(me.end)
        def _():
            for i in range(2):
                for f in me.far:
                    zero(2 * f + i, end_rows, far_rows)

        return 0

    packs = Packs(me, every)
    packs.order(me)
    packs.packers(me, pn_ref, pf_ref)
    for j in range(AHEAD):
        pack(j, 0)
        if j == 0:
            pl.semaphore_wait(barrier, 7)
        send(j)
    lax.fori_loop(AHEAD, n, pack, 0)
    lax.fori_loop(0, n, clear, 0)

    def clear_sums(i, _):
        cols = pl.ds(pl.multiple_of(i * CW, CW), CW)
        for e in range(2):
            gacc[e, :, cols] = jnp.zeros((rows, CW), F32)
            uacc[e, :, cols] = jnp.zeros((rows, CW), F32)
        return 0

    lax.fori_loop(0, tiles, clear_sums, 0)

    def gather(k):
        for i in range(2):
            j = 2 * k + i
            arrived(j, 2 * me.z + 1 - me.c, t)
            arrived(j, 2 * me.near + 1 - me.c, end_rows)
            for f in me.far:

                @pl.when(me.inner)
                def _():
                    arrived(j, 2 * f + 1 - me.c, far_rows)

                @pl.when(me.end)
                def _():
                    arrived(j, 2 * f + 1 - me.c, end_rows)

            for zs in range(4):
                block = dot(a_ref[zs], xall[j, zs * 2 * t : (zs + 1) * 2 * t]).astype(BF16)
                size = rows // 4
                for e in range(2):
                    zbuf[e, zs * size : (zs + 1) * size, i * CW : (i + 1) * CW] = block[e * size : (e + 1) * size]

    def unit(u):
        e, k = lax.rem(u, 2), lax.div(u, 2)

        @pl.when(e == 0)
        def _():
            gather(k)

        def tiles_of(p, last):
            if p % 2 == 0:
                for r in range(p, min(parts, p + 2)):
                    for copy in weights(u, r):
                        copy.wait()
            def tile(i, _):
                here = pl.ds(pl.multiple_of(i * CW, CW), CW)
                cols = pl.ds(pl.multiple_of((starts[p] + i) * CW, CW), CW)
                z = zbuf[e]
                gate = gacc[e, :, cols] + dot(z, wgb[p, :, here])
                up = uacc[e, :, cols] + dot(z, wub[p, :, here])
                if last:
                    h_ref[e, :, cols] = (gate * jax.nn.sigmoid(gate) * up).astype(BF16)
                else:
                    gacc[e, :, cols] = gate
                    uacc[e, :, cols] = up
                return 0

            lax.fori_loop(0, sizes[p], tile, 0, unroll=unroll)

            def start():
                for copy in weights(u + 1, p):
                    copy.start()

            if last:
                pl.when(u + 1 < 2 * nk)(start)
            else:
                start()

        @pl.when(k < nk - 1)
        def _():
            for p in range(parts):
                tiles_of(p, False)

        @pl.when(k == nk - 1)
        def _():
            for p in range(parts):
                tiles_of(p, True)

    def relay(j):
        @pl.when(j + AHEAD < n)
        def _():
            send(j + AHEAD)

        @pl.when(j < n)
        def _():
            @pl.when(me.inner)
            def _():
                for i, slot in enumerate(far_slots):
                    arrived(j, slot, far_rows)
                    forward(j, 6 + i, slot, end_rows, nearby).start()
                    forward(j, 4 + i, slot, far_rows, partner).start()

            arrived(j, near_slot, end_rows)
            forward(j, 3, near_slot, end_rows, partner).start()

        @pl.when(jnp.logical_and(me.end, jnp.logical_and(j >= 1, j <= n)))
        def _():
            for i, slot in enumerate(far_slots):
                arrived(j - 1, slot, end_rows)
                forward(j - 1, 4 + i, slot, end_rows, partner).start()

    def step(j, _):
        relay(j)

        @pl.when(j >= 3)
        def _():
            unit(j - 3)

        return 0

    relay(jnp.int32(0))
    packs.matrices(me, slots, a_ref, cw_ref, qn_ref, qf_ref)
    lax.fori_loop(1, n + 3, step, 0)

    def drain(j, _):
        for copy in sends(j):
            copy.wait_send()
        forward(j, 3, near_slot, end_rows, partner).wait_send()

        @pl.when(me.inner)
        def _():
            for i, slot in enumerate(far_slots):
                forward(j, 6 + i, slot, end_rows, nearby).wait_send()
                forward(j, 4 + i, slot, far_rows, partner).wait_send()

        @pl.when(me.end)
        def _():
            for i, slot in enumerate(far_slots):
                forward(j, 4 + i, slot, end_rows, partner).wait_send()

        return 0

    lax.fori_loop(0, n, drain, 0)


def down_kernel(far_rows, end_rows, h_ref, cw_ref, qn_ref, qf_ref, wd_hbm, y_hbm, y_ref, y_sem, o, yd, yn, yf, yr, sd, sn, sf, wdb, wsem, send_sem, dsem, nsem, fsem, rsem, ready):
    me = Place()
    t, d = y_ref.shape
    ff = wd_hbm.shape[1]
    rows = h_ref.shape[1]
    size = rows // 4
    n = d // CW
    depth = wdb.shape[0]
    lag = 5

    def weights(q):
        cols = pl.ds(pl.multiple_of(q * CW, CW), CW)
        slot = lax.rem(q, depth)
        for e in range(2):
            yield pltpu.make_async_copy(wd_hbm.at[e, :, cols], wdb.at[slot, e], wsem.at[slot, e])

    me.greet(ready)
    for q in range(depth - 1):
        for copy in weights(q):
            copy.start()

    partner, nearby = me.dev(me.z, 1 - me.c), me.dev(me.near, me.c)

    def remote(q, kind, src, dst, recv, to):
        return pltpu.make_async_remote_copy(
            src_ref=src, dst_ref=dst, send_sem=send_sem.at[q, kind], recv_sem=recv, device_id=to, device_id_type=MESH
        )

    def to_partner(q):
        return remote(q, 0, sd.at[q], yd.at[q], dsem.at[q], partner)

    def to_near(q):
        return remote(q, 1, sn.at[q], yn.at[q], nsem.at[q], nearby)

    def relay(q, i):
        return remote(q, 2 + i, sf.at[q, i, pl.ds(0, end_rows)], yr.at[q, i], rsem.at[q, i], nearby)

    def to_far(q, i):
        return remote(q, 2 + i, sf.at[q, i], yf.at[q], fsem.at[q], me.dev(me.far[i], me.c))

    def result(q):
        cols = pl.ds(pl.multiple_of(q * CW, CW), CW)
        return pltpu.make_async_copy(y_ref.at[:, cols], y_hbm.at[:, cols], y_sem.at[q])

    def part(q, zs, c, count):
        return dot(cw_ref[zs, pl.ds(pl.multiple_of(c * t, t), count), :], o[q, zs])

    def both(q, zs, count):
        other = yd[q, pl.ds(pl.multiple_of(zs * t, t), count)].astype(F32)
        return part(q, zs, me.c, count) + other

    def step(q, _):
        @pl.when(jnp.logical_and(me.inner, jnp.logical_and(q >= 2, q <= n + 1)))
        def _():
            r = q - 2
            for i, f in enumerate(me.far):
                relay(r, i).wait_recv()
                total = both(r, f, far_rows)
                sf[r, i, 0:end_rows] = (total[:end_rows] + yr[r, i].astype(F32)).astype(BF16)
                if far_rows > end_rows:
                    sf[r, i, end_rows:far_rows] = total[end_rows:].astype(BF16)
                to_far(r, i).start()

        @pl.when(q < n)
        def _():
            for copy in weights(q):
                copy.wait()

            @pl.when(q + depth - 1 < n)
            def _():
                for copy in weights(q + depth - 1):
                    copy.start()

            slot = lax.rem(q, depth)
            for e in range(2):
                block = dot(h_ref[e], wdb[slot, e]).astype(BF16)
                for zs in range(4):
                    o[q, zs, e * size : (e + 1) * size] = block[zs * size : (zs + 1) * size]
            for zs in range(4):
                sd[q, zs * t : (zs + 1) * t] = part(q, zs, 1 - me.c, t).astype(BF16)

            @pl.when(q == 0)
            def _():
                pl.semaphore_wait(ready, 7)

            to_partner(q).start()

        @pl.when(jnp.logical_and(q >= 1, q <= n))
        def _():
            r = q - 1
            to_partner(r).wait_recv()

            @pl.when(me.end)
            def _():
                for i, f in enumerate(me.far):
                    sf[r, i, 0:end_rows] = both(r, f, end_rows).astype(BF16)
                    relay(r, i).start()

            sn[r] = both(r, me.near, end_rows).astype(BF16)
            to_near(r).start()

        @pl.when(q >= lag)
        def _():
            r = q - lag
            to_near(r).wait_recv()
            to_far(r, 0).wait_recv()
            total = both(r, me.z, t)
            total += dot(qn_ref[:, :end_rows], yn[r])
            total += dot(qf_ref[:, :far_rows], yf[r])
            y_ref[:, pl.ds(pl.multiple_of(r * CW, CW), CW)] = total.astype(BF16)
            result(r).start()

        return 0

    lax.fori_loop(0, n + lag, step, 0)

    def drain(q, _):
        result(q).wait()
        to_partner(q).wait_send()
        to_near(q).wait_send()

        @pl.when(me.end)
        def _():
            for i in range(2):
                relay(q, i).wait_send()

        @pl.when(me.inner)
        def _():
            for i in range(2):
                to_far(q, i).wait_send()

        return 0

    lax.fori_loop(0, n, drain, 0)


def moe_kernel(unroll, slots, far_rows, end_rows, x, every, wg, wu, wd, y, h, a, cw, pn, pf, qn, qf, ready, up_wsem, up_send, up_recv, down_wsem, down_send, dsem, nsem, fsem, rsem, y_sem):
    t, d = x.shape
    n, rows, ff = d // CW, h.shape[1], h.shape[2]
    parts = up_wsem.shape[0]
    wide = -(-(ff // CW) // parts) * CW

    def first(xall, sn, sf, zbuf, gacc, uacc, wgb, wub):
        up_kernel(unroll, slots, far_rows, end_rows, x, every, a, cw, pn, pf, qn, qf, wg, wu, h, xall, sn, sf, zbuf, gacc, uacc, wgb, wub, up_wsem, up_send, up_recv)

    pl.run_scoped(
        first,
        pltpu.VMEM((n, 8 * t, CW), BF16),
        pltpu.VMEM((n, end_rows, CW), BF16),
        pltpu.VMEM((n, far_rows, CW), BF16),
        pltpu.VMEM((2, rows, KC), BF16),
        pltpu.VMEM((2, rows, ff), F32),
        pltpu.VMEM((2, rows, ff), F32),
        pltpu.VMEM((parts, KC, wide), BF16),
        pltpu.VMEM((parts, KC, wide), BF16),
    )

    def second(y_stage, o, yd, yn, yf, yr, sd, sn, sf, wdb):
        down_kernel(far_rows, end_rows, h, cw, qn, qf, wd, y, y_stage, y_sem, o, yd, yn, yf, yr, sd, sn, sf, wdb, down_wsem, down_send, dsem, nsem, fsem, rsem, ready)

    pl.run_scoped(
        second,
        pltpu.VMEM((t, d), BF16),
        pltpu.VMEM((n, 4, rows // 2, CW), BF16),
        pltpu.VMEM((n, 4 * t, CW), BF16),
        pltpu.VMEM((n, end_rows, CW), BF16),
        pltpu.VMEM((n, far_rows, CW), BF16),
        pltpu.VMEM((n, 2, end_rows, CW), BF16),
        pltpu.VMEM((n, 4 * t, CW), BF16),
        pltpu.VMEM((n, end_rows, CW), BF16),
        pltpu.VMEM((n, 2, far_rows, CW), BF16),
        pltpu.VMEM((down_wsem.shape[0], 2, ff, CW), BF16),
    )


def moe_call(x, every, w_gate, w_up, w_down, slots, far_rows, end_rows, unroll, ident):
    t, d = x.shape
    ff = w_gate.shape[2]
    n, rows = d // CW, 8 * slots
    parts = min(4, ff // CW)
    vmem, hbm = pl.BlockSpec(memory_space=pltpu.VMEM), pl.BlockSpec(memory_space=pl.ANY)
    return pl.pallas_call(
        functools.partial(moe_kernel, unroll, slots, far_rows, end_rows),
        out_shape=jax.ShapeDtypeStruct((t, d), BF16),
        in_specs=[vmem] * 2 + [hbm] * 3,
        out_specs=hbm,
        scratch_shapes=[
            pltpu.VMEM((2, rows, ff), BF16),
            pltpu.VMEM((4, 4 * slots, 2 * t), BF16),
            pltpu.VMEM((4, 2 * t, 4 * slots), BF16),
            pltpu.VMEM((t, t), BF16),
            pltpu.VMEM((t, t), BF16),
            pltpu.VMEM((t, t), BF16),
            pltpu.VMEM((t, t), BF16),
            pltpu.SemaphoreType.REGULAR,
            pltpu.SemaphoreType.DMA((parts, 2)),
            pltpu.SemaphoreType.DMA((n, 8)),
            pltpu.SemaphoreType.DMA((n, 8)),
            pltpu.SemaphoreType.DMA((3, 2)),
            pltpu.SemaphoreType.DMA((n, 4)),
            pltpu.SemaphoreType.DMA((n,)),
            pltpu.SemaphoreType.DMA((n,)),
            pltpu.SemaphoreType.DMA((n,)),
            pltpu.SemaphoreType.DMA((n, 2)),
            pltpu.SemaphoreType.DMA((n,)),
        ],
        compiler_params=pltpu.CompilerParams(collective_id=ident, has_side_effects=True, vmem_limit_bytes=VMEM_BYTES),
        name=f"moe_{far_rows}_{end_rows}",
    )(x, every, w_gate, w_up, w_down)


def route_call(expert, slot, gate, slots, sizes, several):
    t = expert.shape[1]
    vmem = pl.BlockSpec(memory_space=pltpu.VMEM)
    return pl.pallas_call(
        functools.partial(route_kernel, slots, sizes, several),
        out_shape=[jax.ShapeDtypeStruct((8, 8, t), F32), jax.ShapeDtypeStruct((1, 1), jnp.int32)],
        in_specs=[vmem] * 3,
        out_specs=[vmem, pl.BlockSpec(memory_space=pltpu.SMEM)],
        scratch_shapes=[
            pltpu.VMEM((8, t), F32),
            pltpu.VMEM((8, 128), F32),
            pltpu.VMEM((3, 8, 128), F32),
            pltpu.SemaphoreType.DMA((7,)),
            pltpu.SemaphoreType.DMA((8,)),
            pltpu.SemaphoreType.DMA((3,)),
            pltpu.SemaphoreType.DMA((3,)),
        ],
        compiler_params=pltpu.CompilerParams(collective_id=0, has_side_effects=True),
        name="route",
    )(expert, slot, gate)


def solution(mesh):
    def body(x, expert, slot, gate, w_gate, w_up, w_down):
        x, expert, slot, gate = x[0, 0], expert[0, 0], slot[0, 0], gate[0, 0]
        t = x.shape[0]
        slots = 5 * t * 2 // (4 * 16)
        sizes = [(160, 112), (192, 144), (t, 4 * slots)]
        every, pick = route_call(expert.T, slot.T, gate.T, slots, sizes, mesh.shape["dp"] > 1)

        def branch(i):
            def run(x, w_gate, w_up, w_down):
                far_rows, end_rows = sizes[i]
                return moe_call(x, every, w_gate, w_up, w_down, slots, far_rows, end_rows, i == 0, 1 + i)

            return run

        y = lax.switch(pick[0, 0], [branch(i) for i in range(len(sizes))], x, w_gate, w_up, w_down)
        return y[None, None]

    data, weight = P("dp", "ep", None, None), P("ep", None, None)
    return jax.shard_map(
        body,
        mesh=mesh,
        in_specs=(data, data, data, data, weight, weight, weight),
        out_specs=data,
        check_vma=False,
    )
```
